32 devices in a mesh: dp: 32 (over z, y, x, core), rank: 1.
Axes of the slice: x: 2, y: 2, z: 4, core: 2. Of those that a mesh axis runs over, the one named last changes fastest.
Arguments:
- cloud_x: float32 [64, 65536], P(None, 'dp'), may hold values from -0.6 to 0.6
- cloud_y: float32 [64, 65536], P(None, 'dp'), may hold values from -0.6 to 0.6
- mass_x: float32 [65536], P('dp'), may hold values from 0.25 to 4
- mass_y: float32 [65536], P('dp'), may hold values from 0.25 to 4
- left_start: float32 [256, 65536], P('rank', 'dp'), may hold values from 0.25 to 204.8
- right_start: float32 [256, 65536], P('rank', 'dp'), may hold values from 0.25 to 204.8
- weight_start: float32 [256], P('rank'), may hold values from 0.25 to 4
Outputs:
- left_factor: float32 [256, 65536], P('rank', 'dp')
- right_factor: float32 [256, 65536], P('rank', 'dp')
- rank_weights: float32 [256], P('rank')
The draws below stay inside these ranges and needn't reach their ends.
All inputs are finite; a program needn't handle non-finite values.
Results may differ from the reference program's by a relative error of at most 0.0003.
Values sent between devices are 32-bit elements; how exact they have to be, the bound alone decides.
No kernel may reach another device: no remote copies, remote signals or barrier semaphores. Data moves between devices by JAX's collectives and lax.ppermute only.
A program may use at most 64 MiB of HBM per device.

```python
import math
import jax
import jax.numpy as jnp
from jax import lax

DIM = 64
RANK = 256
INNER = 4
MIRROR = 3
N = 65536


def cluster_layout(key):
    centres = jax.random.normal(jax.random.fold_in(key, 7101), (DIM, RANK), jnp.float32) * jnp.sqrt(0.6 / DIM)
    shifted = centres + jax.random.normal(jax.random.fold_in(key, 7102), (DIM, RANK), jnp.float32) * jnp.sqrt(0.2 / DIM)
    member_x = jax.random.randint(jax.random.fold_in(key, 7103), (N,), 0, RANK).astype(jnp.int32)
    member_y = jax.random.randint(jax.random.fold_in(key, 7104), (N,), 0, RANK).astype(jnp.int32)
    return (centres, shifted, member_x, member_y)


def cloud_points(key, centres, member, salt):
    base = jnp.take(centres, member, axis=1)
    noise_key = jax.random.fold_in(key, salt)
    noise = jax.random.normal(noise_key, (DIM, N), jnp.float32) * jnp.sqrt(0.5 / DIM)
    return jnp.clip(base + noise, -0.6, 0.6)


def factor_start(key, member, salt):
    rest = jnp.exp(jax.random.uniform(jax.random.fold_in(key, salt), (RANK, N), jnp.float32, jnp.log(0.25), jnp.log(4.0)))
    own = RANK * jnp.exp(jax.random.uniform(jax.random.fold_in(key, salt + 1), (RANK, N), jnp.float32, jnp.log(0.25), jnp.log(0.8)))
    match = jnp.arange(RANK, dtype=jnp.int32)[:, None] == member[None, :]
    return jnp.where(match, own, rest)


def draw_cloud_x(key, part):
    centres, shifted, member_x, member_y = cluster_layout(key)
    return cloud_points(key, centres, member_x, 7201)


def draw_cloud_y(key, part):
    centres, shifted, member_x, member_y = cluster_layout(key)
    return cloud_points(key, shifted, member_y, 7301)


def draw_left_start(key, part):
    centres, shifted, member_x, member_y = cluster_layout(key)
    return factor_start(key, member_x, 7401)


def draw_right_start(key, part):
    centres, shifted, member_x, member_y = cluster_layout(key)
    return factor_start(key, member_y, 7501)


def level_of(key, extent, shards, least, largest):
    def one(dim, shards_of):
        steps = jax.random.uniform(jax.random.fold_in(jax.random.fold_in(key, 6), dim), (shards_of,), jnp.float32, least / len(shards), largest / len(shards))
        return jnp.repeat(jnp.exp(steps), extent[dim] // shards_of).reshape((-1,) + (1,) * (len(extent) - dim - 1))

    gain = one(*shards[0])
    for cut in shards[1:]:
        gain = gain * one(*cut)
    return gain


def setup_inputs(seed: int = 0) -> dict:
    key_of = jax.random.split(jax.random.key(seed), 8)
    cloud_x = draw_cloud_x(jax.random.fold_in(key_of[7], 71), 0)
    cloud_y = draw_cloud_y(jax.random.fold_in(key_of[7], 71), 0)
    mass_x = jnp.clip(jnp.exp(math.log(4.0) - 2.7725887 * jax.random.uniform(key_of[2], (N,), jnp.float32) ** level_of(key_of[2], (N,), ((0, 32),), -0.2, 0.2)), 0.25, 4.0)
    mass_y = jnp.clip(jnp.exp(math.log(4.0) - 2.7725887 * jax.random.uniform(key_of[3], (N,), jnp.float32) ** level_of(key_of[3], (N,), ((0, 32),), -0.2, 0.2)), 0.25, 4.0)
    left_start = draw_left_start(jax.random.fold_in(key_of[7], 71), 0)
    right_start = draw_right_start(jax.random.fold_in(key_of[7], 71), 0)
    weight_start = jnp.clip(jnp.exp(jax.random.uniform(key_of[6], (RANK,), jnp.float32, math.log(0.25), math.log(4.0))), 0.25, 4.0)
    return dict(cloud_x=cloud_x, cloud_y=cloud_y, mass_x=mass_x, mass_y=mass_y, left_start=left_start, right_start=right_start, weight_start=weight_start)


exact_mode = lax.Precision.HIGHEST
step_size = 2.0


def project(kernel_left, kernel_right, kernel_weight, left_mass, right_mass):
    scale_left = jnp.ones((RANK,), jnp.float32)
    scale_right = jnp.ones((RANK,), jnp.float32)
    for repeat in range(INNER):
        point_left = left_mass / jnp.dot(scale_left, kernel_left, precision=exact_mode)
        point_right = right_mass / jnp.dot(scale_right, kernel_right, precision=exact_mode)
        column_left = jnp.dot(kernel_left, point_left, precision=exact_mode)
        column_right = jnp.dot(kernel_right, point_right, precision=exact_mode)
        weights = jnp.cbrt(kernel_weight * scale_left * column_left * scale_right * column_right)
        scale_left = weights / column_left
        scale_right = weights / column_right
    left = point_left[None, :] * kernel_left * scale_left[:, None]
    right = point_right[None, :] * kernel_right * scale_right[:, None]
    return left, right, weights


def moments(cloud, factor):
    product = jnp.dot(cloud, factor.T, precision=exact_mode)
    square = jnp.dot(factor, jnp.sum(cloud * cloud, axis=0), precision=exact_mode)
    column = jnp.sum(factor, axis=1)
    return product, square, column


def reference(cloud_x, cloud_y, mass_x, mass_y, left_start, right_start, weight_start):
    left_mass = mass_x * (N / jnp.sum(mass_x))
    right_mass = mass_y * (N / jnp.sum(mass_y))
    left, right, weights = project(left_start, right_start, weight_start, left_mass, right_mass)
    for outer in range(MIRROR):
        prod_x, square_x, sums_q = moments(cloud_x, left)
        prod_y, square_y, sums_r = moments(cloud_y, right)
        grad_q = square_y / weights
        grad_r = square_x / weights
        grad_g = -(square_x * sums_r + sums_q * square_y - 2.0 * jnp.sum(prod_x * prod_y, axis=0)) / (weights * weights)
        mean_q = jnp.sum(grad_q) / RANK
        mean_r = jnp.sum(grad_r) / RANK
        mean_g = jnp.sum(grad_g) / RANK
        field_q = (grad_q - mean_q)[:, None] - 2.0 * jnp.dot(prod_y.T, cloud_x, precision=exact_mode) / weights[:, None]
        field_r = (grad_r - mean_r)[:, None] - 2.0 * jnp.dot(prod_x.T, cloud_y, precision=exact_mode) / weights[:, None]
        kernel_left = left * jnp.exp(-step_size * field_q)
        kernel_right = right * jnp.exp(-step_size * field_r)
        kernel_weight = weights * jnp.exp(-step_size * (grad_g - mean_g))
        left, right, weights = project(kernel_left, kernel_right, kernel_weight, left_mass, right_mass)
    return RANK * left, RANK * right, (RANK / N) * weights
```

```python
import jax
import jax.numpy as jnp
from jax import lax
from jax.sharding import PartitionSpec as P

RANK = 256
INNER = 4
MIRROR = 3


exact_mode = lax.Precision.HIGHEST
step_size = 2.0


def total_small(part):
    count = lax.axis_size("dp")
    parts = lax.all_to_all(jnp.broadcast_to(part[None], (count,) + part.shape), "dp", 0, 0)
    return jnp.sum(parts, axis=0)


def total_large(part):
    count = lax.axis_size("dp")
    size = part.shape[0]
    piece = -(-size // (count * 128)) * 128
    padded = jnp.pad(part, (0, piece * count - size)).reshape(count, 1, piece)
    mine = jnp.sum(lax.all_to_all(padded, "dp", 0, 0), axis=0)
    parts = lax.all_to_all(jnp.broadcast_to(mine[None], (count, 1, piece)), "dp", 0, 0)
    return parts.reshape(-1)[:size]


def over_rank(value):
    return lax.psum(value, "rank") if lax.axis_size("rank") > 1 else value


def shards(cloud_x, cloud_y, mass_x, mass_y, left_start, right_start, weight_start):
    ranks_local = left_start.shape[0]
    points_dev = left_start.shape[1]
    dim = cloud_x.shape[0]
    total_count = float(points_dev * lax.axis_size("dp"))
    square_x = jnp.sum(cloud_x * cloud_x, axis=0)
    square_y = jnp.sum(cloud_y * cloud_y, axis=0)

    def rows(scale, kernel):
        return over_rank(jnp.sum(scale[:, None] * kernel, axis=0))

    def columns(kernel, point):
        return jnp.sum(kernel * point[None, :], axis=1)

    left_mass, right_mass = mass_x, mass_y
    kernel_left, kernel_right, kernel_weight = left_start, right_start, weight_start
    for outer in range(MIRROR + 1):
        scale_left = jnp.ones((ranks_local,), jnp.float32)
        scale_right = jnp.ones((ranks_local,), jnp.float32)
        for repeat in range(INNER):
            point_left = left_mass / rows(scale_left, kernel_left)
            point_right = right_mass / rows(scale_right, kernel_right)
            if repeat == INNER - 1 and outer < MIRROR:
                break
            column_left = columns(kernel_left, point_left)
            column_right = columns(kernel_right, point_right)
            if outer == 0 and repeat == 0:
                sums = jnp.stack([jnp.sum(mass_x), jnp.sum(mass_y)])
                packed = total_small(jnp.concatenate([column_left, column_right, sums])[None])[0]
                factor_x = total_count / packed[2 * ranks_local]
                factor_y = total_count / packed[2 * ranks_local + 1]
                left_mass = mass_x * factor_x
                right_mass = mass_y * factor_y
                column_left = packed[:ranks_local] * factor_x
                column_right = packed[ranks_local : 2 * ranks_local] * factor_y
            else:
                packed = total_small(jnp.concatenate([column_left, column_right])[None])[0]
                column_left = packed[:ranks_local]
                column_right = packed[ranks_local:]
            weights = jnp.cbrt(
                kernel_weight * scale_left * column_left * scale_right * column_right
            )
            scale_left = weights / column_left
            scale_right = weights / column_right
        if outer == MIRROR:
            break
        plan_left = kernel_left * point_left[None, :] * scale_left[:, None]
        plan_right = kernel_right * point_right[None, :] * scale_right[:, None]
        packed = total_large(
            jnp.concatenate(
                [
                    jnp.dot(cloud_x, plan_left.T, precision=exact_mode).reshape(-1),
                    jnp.dot(cloud_y, plan_right.T, precision=exact_mode).reshape(-1),
                    jnp.sum(plan_left * square_x[None, :], axis=1),
                    jnp.sum(plan_right * square_y[None, :], axis=1),
                    jnp.sum(plan_left, axis=1),
                    jnp.sum(plan_right, axis=1),
                ]
            )
        )
        packed = packed.reshape(2 * dim + 4, ranks_local)
        column_left, column_right = packed[2 * dim + 2], packed[2 * dim + 3]
        weights = jnp.cbrt(kernel_weight * column_left * column_right)
        mean_x = packed[:dim] / column_left
        mean_y = packed[dim : 2 * dim] / column_right
        grad_q = packed[2 * dim + 1] / column_right
        grad_r = packed[2 * dim] / column_left
        grad_g = -(grad_r + grad_q - 2.0 * jnp.sum(mean_x * mean_y, axis=0))
        centre = over_rank(jnp.stack([jnp.sum(grad_q), jnp.sum(grad_r), jnp.sum(grad_g)])) / RANK
        field_q = (grad_q - centre[0])[:, None] - 2.0 * jnp.dot(mean_y.T, cloud_x, precision=exact_mode)
        field_r = (grad_r - centre[1])[:, None] - 2.0 * jnp.dot(mean_x.T, cloud_y, precision=exact_mode)
        kernel_left = plan_left * (weights / column_left)[:, None] * jnp.exp(-step_size * field_q)
        kernel_right = plan_right * (weights / column_right)[:, None] * jnp.exp(-step_size * field_r)
        kernel_weight = weights * jnp.exp(-step_size * (grad_g - centre[2]))
    left = point_left[None, :] * kernel_left * scale_left[:, None]
    right = point_right[None, :] * kernel_right * scale_right[:, None]
    return (RANK * left, RANK * right, weights * (RANK / total_count))


def solution(mesh):
    in_specs = (
        P(None, "dp"),
        P(None, "dp"),
        P("dp"),
        P("dp"),
        P("rank", "dp"),
        P("rank", "dp"),
        P("rank"),
    )
    out_specs = (P("rank", "dp"), P("rank", "dp"), P("rank"))
    return jax.shard_map(shards, mesh=mesh, in_specs=in_specs, out_specs=out_specs, check_vma=False)
```

```python
import functools

import jax
import jax.numpy as jnp
from jax import lax
from jax.experimental import pallas as pl
from jax.experimental.pallas import tpu as pltpu
from jax.sharding import PartitionSpec as P

RANK = 256
INNER = 4
MIRROR = 3


exact_mode = lax.Precision.HIGHEST
step_size = 2.0


def total_small(part):
    count = lax.axis_size("dp")
    parts = lax.all_to_all(jnp.broadcast_to(part[None], (count,) + part.shape), "dp", 0, 0)
    return jnp.sum(parts, axis=0)


def total_large(part):
    count = lax.axis_size("dp")
    size = part.shape[0]
    piece = -(-size // (count * 128)) * 128
    padded = jnp.pad(part, (0, piece * count - size)).reshape(count, 1, piece)
    mine = jnp.sum(lax.all_to_all(padded, "dp", 0, 0), axis=0)
    parts = lax.all_to_all(jnp.broadcast_to(mine[None], (count, 1, piece)), "dp", 0, 0)
    return parts.reshape(-1)[:size]


def over_rank(value):
    return lax.psum(value, "rank") if lax.axis_size("rank") > 1 else value


def shards(cloud_x, cloud_y, mass_x, mass_y, left_start, right_start, weight_start):
    ranks_local = left_start.shape[0]
    points_dev = left_start.shape[1]
    dim = cloud_x.shape[0]
    total_count = float(points_dev * lax.axis_size("dp"))
    square_x = jnp.sum(cloud_x * cloud_x, axis=0)
    square_y = jnp.sum(cloud_y * cloud_y, axis=0)

    def rows(scale, kernel):
        return over_rank(jnp.sum(scale[:, None] * kernel, axis=0))

    def columns(kernel, point):
        return jnp.sum(kernel * point[None, :], axis=1)

    left_mass, right_mass = mass_x, mass_y
    kernel_left, kernel_right, kernel_weight = left_start, right_start, weight_start
    for outer in range(MIRROR + 1):
        scale_left = jnp.ones((ranks_local,), jnp.float32)
        scale_right = jnp.ones((ranks_local,), jnp.float32)
        for repeat in range(INNER):
            point_left = left_mass / rows(scale_left, kernel_left)
            point_right = right_mass / rows(scale_right, kernel_right)
            if repeat == INNER - 1 and outer < MIRROR:
                break
            column_left = columns(kernel_left, point_left)
            column_right = columns(kernel_right, point_right)
            if outer == 0 and repeat == 0:
                sums = jnp.stack([jnp.sum(mass_x), jnp.sum(mass_y)])
                packed = total_small(jnp.concatenate([column_left, column_right, sums])[None])[0]
                factor_x = total_count / packed[2 * ranks_local]
                factor_y = total_count / packed[2 * ranks_local + 1]
                left_mass = mass_x * factor_x
                right_mass = mass_y * factor_y
                column_left = packed[:ranks_local] * factor_x
                column_right = packed[ranks_local : 2 * ranks_local] * factor_y
            else:
                packed = total_small(jnp.concatenate([column_left, column_right])[None])[0]
                column_left = packed[:ranks_local]
                column_right = packed[ranks_local:]
            weights = jnp.cbrt(
                kernel_weight * scale_left * column_left * scale_right * column_right
            )
            scale_left = weights / column_left
            scale_right = weights / column_right
        if outer == MIRROR:
            break
        plan_left = kernel_left * point_left[None, :] * scale_left[:, None]
        plan_right = kernel_right * point_right[None, :] * scale_right[:, None]
        packed = total_large(
            jnp.concatenate(
                [
                    jnp.dot(cloud_x, plan_left.T, precision=exact_mode).reshape(-1),
                    jnp.dot(cloud_y, plan_right.T, precision=exact_mode).reshape(-1),
                    jnp.sum(plan_left * square_x[None, :], axis=1),
                    jnp.sum(plan_right * square_y[None, :], axis=1),
                    jnp.sum(plan_left, axis=1),
                    jnp.sum(plan_right, axis=1),
                ]
            )
        )
        packed = packed.reshape(2 * dim + 4, ranks_local)
        column_left, column_right = packed[2 * dim + 2], packed[2 * dim + 3]
        weights = jnp.cbrt(kernel_weight * column_left * column_right)
        mean_x = packed[:dim] / column_left
        mean_y = packed[dim : 2 * dim] / column_right
        grad_q = packed[2 * dim + 1] / column_right
        grad_r = packed[2 * dim] / column_left
        grad_g = -(grad_r + grad_q - 2.0 * jnp.sum(mean_x * mean_y, axis=0))
        centre = over_rank(jnp.stack([jnp.sum(grad_q), jnp.sum(grad_r), jnp.sum(grad_g)])) / RANK
        field_q = (grad_q - centre[0])[:, None] - 2.0 * jnp.dot(mean_y.T, cloud_x, precision=exact_mode)
        field_r = (grad_r - centre[1])[:, None] - 2.0 * jnp.dot(mean_x.T, cloud_y, precision=exact_mode)
        kernel_left = plan_left * (weights / column_left)[:, None] * jnp.exp(-step_size * field_q)
        kernel_right = plan_right * (weights / column_right)[:, None] * jnp.exp(-step_size * field_r)
        kernel_weight = weights * jnp.exp(-step_size * (grad_g - centre[2]))
    left = point_left[None, :] * kernel_left * scale_left[:, None]
    right = point_right[None, :] * kernel_right * scale_right[:, None]
    return (RANK * left, RANK * right, weights * (RANK / total_count))


LANES = 128
HIGH = jnp.float32
HALF = jnp.bfloat16


def halves(value):
    high = value.astype(HALF)
    return high, (value - high.astype(HIGH)).astype(HALF)


def cube_root(value):
    root = jnp.exp(jnp.log(value) * (1.0 / 3.0))
    return root - (root - value / (root * root)) * (1.0 / 3.0)


def to_columns(rows):
    return jnp.concatenate(
        [jnp.transpose(jnp.broadcast_to(rows[j : j + 1], (LANES, LANES))) for j in range(rows.shape[0])],
        axis=0,
    )


def to_rows(block):
    return jnp.concatenate(
        [
            jnp.sum(jnp.transpose(block[j : j + LANES]), axis=0, keepdims=True)
            for j in range(0, block.shape[0], LANES)
        ],
        axis=0,
    )


def wide(column, width):
    return jnp.concatenate([column] * (width // LANES), axis=1)


def fold(block):
    total = block[:, :LANES]
    for j in range(LANES, block.shape[1], LANES):
        total = total + block[:, j : j + LANES]
    return total


def column_pass(kernel_ref, column, mass_ref, point_ref, width, arrivals=()):
    total = None
    for start in range(0, kernel_ref.shape[1], width):
        part = pl.ds(start, width)
        if arrivals:
            arrivals[start // width].wait()
        block = kernel_ref[:, part]
        scaled = block if column is None else block * wide(column, width)
        point = mass_ref[:, part] / jnp.sum(scaled, axis=0, keepdims=True)
        if point_ref is not None:
            point_ref[:, part] = point
        piece = fold(kernel_ref[:, part] * point)
        total = piece if total is None else total + piece
    return total


def send(out_ref, left, right):
    packed = jnp.concatenate([to_rows(left), to_rows(right)], axis=0)
    out_ref[...] = jnp.broadcast_to(packed[None], out_ref.shape)


def receive(parts_ref, weight_ref, scale_ref, count):
    rows = weight_ref.shape[0]
    totals = jnp.sum(parts_ref[...], axis=0)
    column_left, column_right = totals[:rows], totals[rows:]
    factors = None
    if scale_ref is None:
        factors = [count / jnp.sum(c, keepdims=True) for c in (column_left, column_right)]
        column_left = column_left * factors[0]
        column_right = column_right * factors[1]
        weights = cube_root(weight_ref[...] * column_left * column_right)
    else:
        weights = cube_root(
            weight_ref[...] * scale_ref[:rows] * column_left * scale_ref[rows:] * column_right
        )
    return weights, weights / column_left, weights / column_right, factors


def first_kernel(
    left_hbm, right_hbm, mass_x_hbm, mass_y_hbm, out_ref, left_ref, right_ref, mass_x_ref, mass_y_ref, sems, *, width
):
    points = left_ref.shape[1]
    small = [
        pltpu.make_async_copy(mass_x_hbm, mass_x_ref, sems.at[0]),
        pltpu.make_async_copy(mass_y_hbm, mass_y_ref, sems.at[1]),
    ]
    large = []
    for source, target in ((left_hbm, left_ref), (right_hbm, right_ref)):
        for start in range(0, points, width):
            part = pl.ds(start, width)
            sem = sems.at[2 + len(large)]
            large.append(pltpu.make_async_copy(source.at[:, part], target.at[:, part], sem))
    for copy in small + large:
        copy.start()
    for copy in small:
        copy.wait()
    half = len(large) // 2
    send(
        out_ref,
        column_pass(left_ref, None, mass_x_ref, None, width, large[:half]),
        column_pass(right_ref, None, mass_y_ref, None, width, large[half:]),
    )


def step_kernel(*refs, width, count, first, fresh, keep):
    refs = list(refs)
    if first:
        sems, buffer_x, buffer_y = refs.pop(), refs.pop(), refs.pop()
        clouds = [
            pltpu.make_async_copy(source, target, sems.at[j])
            for j, (source, target) in enumerate(zip(refs[:2], (buffer_x, buffer_y)))
        ]
        del refs[:2]
        for copy in clouds:
            copy.start()
    parts_ref, weight_ref = refs[:2]
    del refs[:2]
    scale_in = None if fresh else refs.pop(0)
    left_ref, right_ref, mass_x_ref, mass_y_ref, out_ref, scale_ref = refs[:6]
    del refs[:6]
    if fresh and not first:
        rows = weight_ref.shape[0]
        totals = jnp.sum(parts_ref[...], axis=0)
        weights = cube_root(weight_ref[...] * totals[:rows] * totals[rows:])
        scale_left, scale_right, factors = weights / totals[:rows], weights / totals[rows:], None
    else:
        _, scale_left, scale_right, factors = receive(parts_ref, weight_ref, scale_in, count)
    scale_ref[...] = jnp.concatenate([scale_left, scale_right], axis=0)
    if first:
        new_x_ref, new_y_ref = refs[:2]
        del refs[:2]
        new_x_ref[...] = mass_x_ref[...] * factors[0]
        new_y_ref[...] = mass_y_ref[...] * factors[1]
        mass_x_ref, mass_y_ref = new_x_ref, new_y_ref
    point_x_ref, point_y_ref = refs[:2] if keep else (None, None)
    send(
        out_ref,
        column_pass(left_ref, to_columns(scale_left), mass_x_ref, point_x_ref, width),
        column_pass(right_ref, to_columns(scale_right), mass_y_ref, point_y_ref, width),
    )
    if first:
        for copy in clouds:
            copy.wait()
        halve_cloud(buffer_x, refs[0], refs[1], width // 2)
        halve_cloud(buffer_y, refs[2], refs[3], width // 2)


def halve_cloud(cloud_ref, tall_ref, flat_ref, width):
    dim = cloud_ref.shape[0]
    for start in range(0, cloud_ref.shape[1], width):
        part = pl.ds(start, width)
        points = cloud_ref[:, part]
        high, low = halves(points)
        flat_ref[:, part] = jnp.concatenate([high, low, high, low], axis=0)
        square = jnp.sum(points * points, axis=0, keepdims=True)
        lines = lax.broadcasted_iota(jnp.int32, (LANES - dim, width), 0)
        rest = jnp.where(lines == 0, square, jnp.where(lines == 1, 1.0, 0.0))
        tall = jnp.concatenate([points, rest], axis=0)
        for j in range(0, width, LANES):
            high, low = halves(jnp.transpose(tall[:, j : j + LANES]))
            tall_ref[pl.ds(start + j, LANES), :] = jnp.concatenate([high, low], axis=1)


def moment_side(kernel_ref, column, mass_ref, tall_ref, plan_ref, width):
    total = None
    for start in range(0, kernel_ref.shape[1], width):
        part = pl.ds(start, width)
        scaled = kernel_ref[:, part] * wide(column, width)
        plan = scaled * (mass_ref[:, part] / jnp.sum(scaled, axis=0, keepdims=True))
        plan_ref[:, part] = plan
        high, low = halves(plan)
        tall = tall_ref[part, :]
        piece = jnp.dot(high, tall, preferred_element_type=HIGH)
        piece = piece + jnp.dot(low, tall, preferred_element_type=HIGH)
        total = piece if total is None else total + piece
    return fold(total)


def moment_kernel(
    parts_ref, weight_ref, scale_ref, left_ref, right_ref, mass_x_ref, mass_y_ref, tall_x_ref, tall_y_ref,
    out_ref, plan_left_ref, plan_right_ref, *, width, count, dim,
):
    _, scale_left, scale_right, _ = receive(parts_ref, weight_ref, scale_ref, count)
    left = moment_side(left_ref, to_columns(scale_left), mass_x_ref, tall_x_ref, plan_left_ref, width)
    right = moment_side(right_ref, to_columns(scale_right), mass_y_ref, tall_y_ref, plan_right_ref, width)
    ranks = left.shape[0]
    lane = lax.broadcasted_iota(jnp.int32, (ranks, LANES), 1)
    out_ref[:ranks] = jnp.where(lane < dim, left, pltpu.roll(right, dim, 1))
    extra = jnp.where(lane < 2, pltpu.roll(left, LANES - dim, 1), pltpu.roll(right, LANES - dim + 2, 1))
    for j in range(ranks // LANES):
        lines = jnp.transpose(extra[j * LANES : (j + 1) * LANES])
        out_ref[ranks + 8 * j : ranks + 8 * j + 8] = lines[:8]
    used = ranks + 8 * (ranks // LANES)
    out_ref[used:] = jnp.zeros((out_ref.shape[0] - used, LANES), HIGH)


def mirror_kernel(
    sums_ref, weight_ref, plan_left_ref, plan_right_ref, mass_x_ref, mass_y_ref, flat_x_ref, flat_y_ref,
    out_ref, left_ref, right_ref, weight_out_ref, *, width, dim,
):
    ranks = plan_left_ref.shape[0]
    tiles = ranks // LANES
    lane = lax.broadcasted_iota(jnp.int32, (ranks, LANES), 1)
    lines = [sums_ref[ranks + 8 * j : ranks + 8 * j + 8] for j in range(tiles)]
    weights = cube_root(
        weight_ref[...]
        * jnp.concatenate([x[1:2] for x in lines], axis=0)
        * jnp.concatenate([x[3:4] for x in lines], axis=0)
    )
    blank = jnp.zeros((LANES - 16, LANES), HIGH)
    extra = jnp.concatenate(
        [
            jnp.transpose(
                jnp.concatenate(
                    [lines[j], jnp.broadcast_to(weights[j : j + 1], (8, LANES)), blank], axis=0
                )
            )
            for j in range(tiles)
        ],
        axis=0,
    )
    column_left, column_right, weight = extra[:, 1:2], extra[:, 3:4], extra[:, 8:9]
    grad_r, grad_q = extra[:, 0:1] / column_left, extra[:, 2:3] / column_right
    mean = sums_ref[:ranks] / jnp.where(lane < dim, column_left, column_right)
    swapped = pltpu.roll(mean, dim, 1)
    cross = jnp.sum(mean * swapped, axis=1, keepdims=True)
    grad_g = cross - grad_r - grad_q
    inverse = 1.0 / ranks
    shift_g = grad_g - jnp.sum(grad_g, axis=0, keepdims=True) * inverse
    shift_q = grad_q - jnp.sum(grad_q, axis=0, keepdims=True) * inverse
    shift_r = grad_r - jnp.sum(grad_r, axis=0, keepdims=True) * inverse
    moved = jnp.broadcast_to(weight * jnp.exp(-step_size * shift_g), (ranks, LANES))
    weight_out_ref[...] = jnp.concatenate(
        [jnp.transpose(moved[j * LANES : (j + 1) * LANES])[:1] for j in range(tiles)], axis=0
    )

    def side(points, factor, shift, plan_ref, flat_ref, mass_ref, kernel_ref):
        high, low = halves(points * (2.0 * step_size))
        points = jnp.concatenate([high, low], axis=1)
        factor = jnp.broadcast_to(factor, (ranks, width))
        shift = jnp.broadcast_to(shift * (-step_size), (ranks, width))
        total = None
        for start in range(0, plan_ref.shape[1], width):
            part = pl.ds(start, width)
            field = jnp.dot(points, flat_ref[:, part], preferred_element_type=HIGH) + shift
            kernel = plan_ref[:, part] * factor * jnp.exp(field)
            kernel_ref[:, part] = kernel
            point = mass_ref[:, part] / jnp.sum(kernel, axis=0, keepdims=True)
            piece = fold(kernel * point)
            total = piece if total is None else total + piece
        return total

    left = side(
        jnp.where(lane < dim, swapped, mean), weight / column_left, shift_q,
        plan_left_ref, flat_x_ref, mass_x_ref, left_ref,
    )
    right = side(
        jnp.where(lane < dim, mean, swapped), weight / column_right, shift_r,
        plan_right_ref, flat_y_ref, mass_y_ref, right_ref,
    )
    send(out_ref, left, right)


def combine_kernel(parts_ref, out_ref):
    out_ref[...] = jnp.broadcast_to(jnp.sum(parts_ref[...], axis=0, keepdims=True), out_ref.shape)


def last_kernel(
    parts_ref, weight_ref, scale_ref, left_ref, right_ref, point_x_ref, point_y_ref,
    left_hbm, right_hbm, weight_out_ref, left_out, right_out, sems, *, count, height,
):
    ranks = left_ref.shape[0]
    weights, scale_left, scale_right, _ = receive(parts_ref, weight_ref, scale_ref, count)
    copies = []
    for scale, point_ref, kernel_ref, buffer, target in (
        (scale_left, point_x_ref, left_ref, left_out, left_hbm),
        (scale_right, point_y_ref, right_ref, right_out, right_hbm),
    ):
        column = to_columns(scale) * float(RANK)
        for start in range(0, ranks, height):
            part = pl.ds(start, height)
            factor = wide(column[start : start + height], kernel_ref.shape[1])
            buffer[part] = point_ref[...] * kernel_ref[part] * factor
            copies.append(pltpu.make_async_copy(buffer.at[part], target.at[part], sems.at[len(copies)]))
            copies[-1].start()
    weight_out_ref[...] = weights * (RANK / count)
    for copy in copies:
        copy.wait()


def kernel_shards(cloud_x, cloud_y, mass_x, mass_y, left_start, right_start, weight_start):
    ranks, points = left_start.shape
    dim = cloud_x.shape[0]
    devices = lax.axis_size("dp")
    count = float(points * devices)
    tiles = ranks // LANES
    shape = jax.ShapeDtypeStruct
    small = shape((devices, 2 * tiles, LANES), HIGH)
    scale = shape((2 * tiles, LANES), HIGH)
    weight_shape = shape((tiles, LANES), HIGH)
    line = shape((1, points), HIGH)
    matrix = shape((ranks, points), HIGH)
    lines = -(-(ranks + 8 * tiles) // devices) * devices
    step_width = 512
    width = 256
    height = LANES // 4
    vmem_bytes = 16 * 1024 * 1024

    def call(body, out, *operands, flops, far_in=0, far_out=0, scratch=()):
        near, far = pl.BlockSpec(memory_space=pltpu.VMEM), pl.BlockSpec(memory_space=pltpu.HBM)
        spaces = [far] * far_out + [near] * (len(out) - far_out)
        return pl.pallas_call(
            body,
            out_shape=out,
            in_specs=[far] * far_in + [near] * (len(operands) - far_in),
            out_specs=spaces,
            scratch_shapes=scratch,
            compiler_params=pltpu.CompilerParams(vmem_limit_bytes=vmem_bytes),
            cost_estimate=pl.CostEstimate(flops=flops, bytes_accessed=0, transcendentals=0),
        )(*[pltpu.with_memory_space_constraint(x, pltpu.HBM) for x in operands[:far_in]], *operands[far_in:])

    def exchange(sent):
        return lax.all_to_all(sent, "dp", 0, 0)

    step_flops = 8 * ranks * points
    mass_x, mass_y = mass_x.reshape(1, points), mass_y.reshape(1, points)
    weight = weight_start.reshape(tiles, LANES)
    parts, left, right, mass_x, mass_y = call(
        functools.partial(first_kernel, width=step_width),
        (small, matrix, matrix, line, line),
        left_start, right_start, mass_x, mass_y,
        flops=step_flops,
        far_in=4,
        scratch=[pltpu.SemaphoreType.DMA((2 + 2 * points // step_width,))],
    )
    cloud_scratch = [pltpu.VMEM(cloud_y.shape, HIGH), pltpu.VMEM(cloud_x.shape, HIGH), pltpu.SemaphoreType.DMA((2,))]
    cloud_shapes = (shape((points, 2 * LANES), HALF), shape((4 * dim, points), HALF))
    for outer in range(MIRROR + 1):
        scaling = ()
        for repeat in range(1, INNER):
            parts = exchange(parts)
            if repeat == INNER - 1 and outer < MIRROR:
                break
            first = outer == 0 and repeat == 1
            keep = outer == MIRROR and repeat == INNER - 1
            body = functools.partial(
                step_kernel, width=step_width, count=count, first=first, fresh=repeat == 1, keep=keep
            )
            out = (small, scale) + (line, line) * (first + keep) + (cloud_shapes * 2) * first
            clouds = (cloud_x, cloud_y) * first
            parts, new_scaling, *more = call(
                body, out, *clouds, parts, weight, *scaling, left, right, mass_x, mass_y,
                flops=step_flops,
                far_in=len(clouds),
                scratch=cloud_scratch * first,
            )
            scaling = (new_scaling,)
            if first:
                mass_x, mass_y, tall_x, flat_x, tall_y, flat_y = more
        if outer == MIRROR:
            break
        sent, left, right = call(
            functools.partial(moment_kernel, width=width, count=count, dim=dim),
            (shape((lines, LANES), HIGH), matrix, matrix),
            parts, weight, *scaling, left, right, mass_x, mass_y, tall_x, tall_y,
            flops=step_flops + 16 * ranks * points * LANES,
        )
        sent = exchange(sent.reshape(devices, 1, -1))
        (sent,) = call(combine_kernel, (shape(sent.shape, HIGH),), sent, flops=lines * LANES)
        sums = exchange(sent).reshape(lines, LANES)
        parts, left, right, weight = call(
            functools.partial(mirror_kernel, width=width, dim=dim),
            (small, matrix, matrix, weight_shape),
            sums, weight, left, right, mass_x, mass_y, flat_x, flat_y,
            flops=step_flops + 16 * ranks * points * dim,
        )
    parts = exchange(parts)
    left, right, weights = call(
        functools.partial(last_kernel, count=count, height=height),
        (matrix, matrix, weight_shape),
        parts, weight, *scaling, left, right, *more,
        flops=step_flops,
        far_out=2,
        scratch=[
            pltpu.VMEM((ranks, points), HIGH),
            pltpu.VMEM((ranks, points), HIGH),
            pltpu.SemaphoreType.DMA((2 * ranks // height,)),
        ],
    )
    return (left, right, weights.reshape(ranks))


def device_program(cloud_x, cloud_y, mass_x, mass_y, left_start, right_start, weight_start):
    ranks, points = left_start.shape
    whole = lax.axis_size("rank") == 1 and cloud_x.shape[0] == LANES // 2
    body = kernel_shards if whole and ranks % LANES == 0 and points % 512 == 0 else shards
    return body(cloud_x, cloud_y, mass_x, mass_y, left_start, right_start, weight_start)


def solution(mesh):
    in_specs = (
        P(None, "dp"),
        P(None, "dp"),
        P("dp"),
        P("dp"),
        P("rank", "dp"),
        P("rank", "dp"),
        P("rank"),
    )
    out_specs = (P("rank", "dp"), P("rank", "dp"), P("rank"))
    return jax.shard_map(device_program, mesh=mesh, in_specs=in_specs, out_specs=out_specs, check_vma=False)
```

```python
import functools

import jax
import jax.numpy as jnp
from jax import lax
from jax.experimental import pallas as pl
from jax.experimental.pallas import tpu as pltpu
from jax.sharding import PartitionSpec as P

RANK = 256
INNER = 4
MIRROR = 3


exact_mode = lax.Precision.HIGHEST
step_size = 2.0


def total_small(part):
    count = lax.axis_size("dp")
    parts = lax.all_to_all(jnp.broadcast_to(part[None], (count,) + part.shape), "dp", 0, 0)
    return jnp.sum(parts, axis=0)


def total_large(part):
    count = lax.axis_size("dp")
    size = part.shape[0]
    piece = -(-size // (count * 128)) * 128
    padded = jnp.pad(part, (0, piece * count - size)).reshape(count, 1, piece)
    mine = jnp.sum(lax.all_to_all(padded, "dp", 0, 0), axis=0)
    parts = lax.all_to_all(jnp.broadcast_to(mine[None], (count, 1, piece)), "dp", 0, 0)
    return parts.reshape(-1)[:size]


def over_rank(value):
    return lax.psum(value, "rank") if lax.axis_size("rank") > 1 else value


def shards(cloud_x, cloud_y, mass_x, mass_y, left_start, right_start, weight_start):
    ranks_local = left_start.shape[0]
    points_dev = left_start.shape[1]
    dim = cloud_x.shape[0]
    total_count = float(points_dev * lax.axis_size("dp"))
    square_x = jnp.sum(cloud_x * cloud_x, axis=0)
    square_y = jnp.sum(cloud_y * cloud_y, axis=0)

    def rows(scale, kernel):
        return over_rank(jnp.sum(scale[:, None] * kernel, axis=0))

    def columns(kernel, point):
        return jnp.sum(kernel * point[None, :], axis=1)

    left_mass, right_mass = mass_x, mass_y
    kernel_left, kernel_right, kernel_weight = left_start, right_start, weight_start
    for outer in range(MIRROR + 1):
        scale_left = jnp.ones((ranks_local,), jnp.float32)
        scale_right = jnp.ones((ranks_local,), jnp.float32)
        for repeat in range(INNER):
            point_left = left_mass / rows(scale_left, kernel_left)
            point_right = right_mass / rows(scale_right, kernel_right)
            if repeat == INNER - 1 and outer < MIRROR:
                break
            column_left = columns(kernel_left, point_left)
            column_right = columns(kernel_right, point_right)
            if outer == 0 and repeat == 0:
                sums = jnp.stack([jnp.sum(mass_x), jnp.sum(mass_y)])
                packed = total_small(jnp.concatenate([column_left, column_right, sums])[None])[0]
                factor_x = total_count / packed[2 * ranks_local]
                factor_y = total_count / packed[2 * ranks_local + 1]
                left_mass = mass_x * factor_x
                right_mass = mass_y * factor_y
                column_left = packed[:ranks_local] * factor_x
                column_right = packed[ranks_local : 2 * ranks_local] * factor_y
            else:
                packed = total_small(jnp.concatenate([column_left, column_right])[None])[0]
                column_left = packed[:ranks_local]
                column_right = packed[ranks_local:]
            weights = jnp.cbrt(
                kernel_weight * scale_left * column_left * scale_right * column_right
            )
            scale_left = weights / column_left
            scale_right = weights / column_right
        if outer == MIRROR:
            break
        plan_left = kernel_left * point_left[None, :] * scale_left[:, None]
        plan_right = kernel_right * point_right[None, :] * scale_right[:, None]
        packed = total_large(
            jnp.concatenate(
                [
                    jnp.dot(cloud_x, plan_left.T, precision=exact_mode).reshape(-1),
                    jnp.dot(cloud_y, plan_right.T, precision=exact_mode).reshape(-1),
                    jnp.sum(plan_left * square_x[None, :], axis=1),
                    jnp.sum(plan_right * square_y[None, :], axis=1),
                    jnp.sum(plan_left, axis=1),
                    jnp.sum(plan_right, axis=1),
                ]
            )
        )
        packed = packed.reshape(2 * dim + 4, ranks_local)
        column_left, column_right = packed[2 * dim + 2], packed[2 * dim + 3]
        weights = jnp.cbrt(kernel_weight * column_left * column_right)
        mean_x = packed[:dim] / column_left
        mean_y = packed[dim : 2 * dim] / column_right
        grad_q = packed[2 * dim + 1] / column_right
        grad_r = packed[2 * dim] / column_left
        grad_g = -(grad_r + grad_q - 2.0 * jnp.sum(mean_x * mean_y, axis=0))
        centre = over_rank(jnp.stack([jnp.sum(grad_q), jnp.sum(grad_r), jnp.sum(grad_g)])) / RANK
        field_q = (grad_q - centre[0])[:, None] - 2.0 * jnp.dot(mean_y.T, cloud_x, precision=exact_mode)
        field_r = (grad_r - centre[1])[:, None] - 2.0 * jnp.dot(mean_x.T, cloud_y, precision=exact_mode)
        kernel_left = plan_left * (weights / column_left)[:, None] * jnp.exp(-step_size * field_q)
        kernel_right = plan_right * (weights / column_right)[:, None] * jnp.exp(-step_size * field_r)
        kernel_weight = weights * jnp.exp(-step_size * (grad_g - centre[2]))
    left = point_left[None, :] * kernel_left * scale_left[:, None]
    right = point_right[None, :] * kernel_right * scale_right[:, None]
    return (RANK * left, RANK * right, weights * (RANK / total_count))


LANES = 128
HIGH = jnp.float32
HALF = jnp.bfloat16
LOG2_E = 1.4426950408889634


def halves(value):
    high = value.astype(HALF)
    return high, (value - high.astype(HIGH)).astype(HALF)


def cube_root(value):
    inverse = jnp.exp2(jnp.log2(value) * (-1.0 / 3.0))
    scaled = value * inverse
    inverse = inverse + inverse * (1.0 - scaled * inverse * inverse) * (1.0 / 3.0)
    return value * inverse * inverse


def tree_sum(ref):
    parts = [ref[j] for j in range(ref.shape[0])]
    while len(parts) > 1:
        pairs = [parts[j] + parts[j + 1] for j in range(0, len(parts) - 1, 2)]
        parts = pairs + parts[len(parts) - len(parts) % 2 :]
    return parts[0]


def to_columns(rows):
    return jnp.concatenate(
        [jnp.transpose(jnp.broadcast_to(rows[j : j + 1], (LANES, LANES))) for j in range(rows.shape[0])],
        axis=0,
    )


def to_rows(block):
    return jnp.concatenate(
        [
            jnp.sum(jnp.transpose(block[j : j + LANES]), axis=0, keepdims=True)
            for j in range(0, block.shape[0], LANES)
        ],
        axis=0,
    )


def wide(column, width):
    return jnp.concatenate([column] * (width // LANES), axis=1)


def fold(block):
    total = block[:, :LANES]
    for j in range(LANES, block.shape[1], LANES):
        total = total + block[:, j : j + LANES]
    return total


def points_of(kernel_ref, column, mass_ref, arrivals=()):
    points = []
    for start in range(0, kernel_ref.shape[1], LANES):
        part = pl.ds(start, LANES)
        if arrivals and start % (kernel_ref.shape[1] // len(arrivals)) == 0:
            arrivals[start * len(arrivals) // kernel_ref.shape[1]].wait()
        block = kernel_ref[:, part]
        if column is not None:
            block = block * column
        points.append(mass_ref[:, part] / jnp.sum(block, axis=0, keepdims=True))
    return jnp.concatenate(points, axis=1)


def column_sums(kernel_ref, point):
    spread = jnp.broadcast_to(point, (8, point.shape[1]))
    return jnp.concatenate(
        [fold(kernel_ref[pl.ds(row, 8), :] * spread) for row in range(0, kernel_ref.shape[0], 8)], axis=0
    )


def send(out_ref, left, right):
    packed = jnp.concatenate([to_rows(left), to_rows(right)], axis=0)
    out_ref[...] = jnp.broadcast_to(packed[None], out_ref.shape)


def receive(parts_ref, weight_ref, scale_ref, count):
    rows = weight_ref.shape[0]
    totals = tree_sum(parts_ref)
    column_left, column_right = totals[:rows], totals[rows:]
    factors = None
    if scale_ref is None:
        factors = [count / jnp.sum(c, keepdims=True) for c in (column_left, column_right)]
        column_left = column_left * factors[0]
        column_right = column_right * factors[1]
        weights = cube_root(weight_ref[...] * column_left * column_right)
    else:
        weights = cube_root(
            weight_ref[...] * scale_ref[:rows] * column_left * scale_ref[rows:] * column_right
        )
    return weights, weights / column_left, weights / column_right, factors


def first_kernel(
    left_hbm, right_hbm, mass_x_hbm, mass_y_hbm, cloud_x_hbm, cloud_y_hbm,
    out_ref, left_ref, right_ref, mass_x_ref, mass_y_ref, tall_x_ref, flat_x_ref, tall_y_ref, flat_y_ref,
    cloud_x_ref, cloud_y_ref, sems, cloud_sems, *, width,
):
    points = left_ref.shape[1]
    clouds = [
        pltpu.make_async_copy(cloud_x_hbm, cloud_x_ref, cloud_sems.at[0]),
        pltpu.make_async_copy(cloud_y_hbm, cloud_y_ref, cloud_sems.at[1]),
    ]
    small = [
        pltpu.make_async_copy(mass_x_hbm, mass_x_ref, sems.at[0]),
        pltpu.make_async_copy(mass_y_hbm, mass_y_ref, sems.at[1]),
    ]
    large = []
    for source, target in ((left_hbm, left_ref), (right_hbm, right_ref)):
        for start in range(0, points, width):
            part = pl.ds(start, width)
            sem = sems.at[2 + len(large)]
            large.append(pltpu.make_async_copy(source.at[:, part], target.at[:, part], sem))
    half = len(large) // 2
    for copy in small + large[:half] + clouds + large[half:]:
        copy.start()
    for copy in small:
        copy.wait()
    left = column_sums(left_ref, points_of(left_ref, None, mass_x_ref, large[:half]))
    for copy, source, tall_ref, flat_ref in zip(
        clouds, (cloud_x_ref, cloud_y_ref), (tall_x_ref, tall_y_ref), (flat_x_ref, flat_y_ref)
    ):
        copy.wait()
        halve_cloud(source, tall_ref, flat_ref, width // 2)
    right = None
    for start, copy in zip(range(0, points, width), large[half:]):
        copy.wait()
        part = pl.ds(start, width)
        block = right_ref.at[:, part]
        piece = column_sums(block, points_of(block, None, mass_y_ref.at[:, part]))
        right = piece if right is None else right + piece
    send(out_ref, left, right)


def step_kernel(*refs, count, first, fresh, keep):
    refs = list(refs)
    parts_ref, weight_ref = refs[:2]
    del refs[:2]
    scale_in = None if fresh else refs.pop(0)
    left_ref, right_ref, mass_x_ref, mass_y_ref, out_ref, scale_ref = refs[:6]
    del refs[:6]
    if fresh and not first:
        rows = weight_ref.shape[0]
        totals = tree_sum(parts_ref)
        weights = cube_root(weight_ref[...] * totals[:rows] * totals[rows:])
        scale_left, scale_right, factors = weights / totals[:rows], weights / totals[rows:], None
    else:
        _, scale_left, scale_right, factors = receive(parts_ref, weight_ref, scale_in, count)
    scale_ref[...] = jnp.concatenate([scale_left, scale_right], axis=0)
    if first:
        new_x_ref, new_y_ref = refs[:2]
        del refs[:2]
        new_x_ref[...] = mass_x_ref[...] * factors[0]
        new_y_ref[...] = mass_y_ref[...] * factors[1]
        mass_x_ref, mass_y_ref = new_x_ref, new_y_ref
    point_x_ref, point_y_ref = refs[:2] if keep else (None, None)
    point_x = points_of(left_ref, to_columns(scale_left), mass_x_ref)
    point_y = points_of(right_ref, to_columns(scale_right), mass_y_ref)
    send(out_ref, column_sums(left_ref, point_x), column_sums(right_ref, point_y))
    if keep:
        point_x_ref[...] = point_x
        point_y_ref[...] = point_y


def halve_cloud(cloud_ref, tall_ref, flat_ref, width):
    dim = cloud_ref.shape[0]
    for start in range(0, cloud_ref.shape[1], width):
        part = pl.ds(start, width)
        points = cloud_ref[:, part]
        high, low = halves(points)
        lines = lax.broadcasted_iota(jnp.int32, (dim, width), 0)
        ones = jnp.where(lines < 3, 1.0, 0.0).astype(HALF)
        flat_ref[:, part] = jnp.concatenate([high, low, high, ones], axis=0)
        square = jnp.sum(points * points, axis=0, keepdims=True)
        lines = lax.broadcasted_iota(jnp.int32, (LANES - dim, width), 0)
        rest = jnp.where(lines == 0, square, jnp.where(lines == 1, 1.0, 0.0))
        tall = jnp.concatenate([points, rest], axis=0)
        for j in range(0, width, LANES):
            high, low = halves(jnp.transpose(tall[:, j : j + LANES]))
            tall_ref[pl.ds(start + j, LANES), :] = jnp.concatenate([high, low], axis=1)


def moment_side(kernel_ref, column, mass_ref, tall_ref, plan_ref, width):
    total = None
    for start in range(0, kernel_ref.shape[1], width):
        part = pl.ds(start, width)
        scaled = kernel_ref[:, part] * wide(column, width)
        plan = scaled * (mass_ref[:, part] / jnp.sum(scaled, axis=0, keepdims=True))
        plan_ref[:, part] = plan
        high, low = halves(plan)
        tall = tall_ref[part, :]
        piece = jnp.dot(high, tall, preferred_element_type=HIGH)
        piece = piece + jnp.dot(low, tall, preferred_element_type=HIGH)
        total = piece if total is None else total + piece
    return fold(total)


def moment_kernel(
    parts_ref, weight_ref, scale_ref, left_ref, right_ref, mass_x_ref, mass_y_ref, tall_x_ref, tall_y_ref,
    out_ref, plan_left_ref, plan_right_ref, *, width, count, dim,
):
    _, scale_left, scale_right, _ = receive(parts_ref, weight_ref, scale_ref, count)
    left = moment_side(left_ref, to_columns(scale_left), mass_x_ref, tall_x_ref, plan_left_ref, width)
    right = moment_side(right_ref, to_columns(scale_right), mass_y_ref, tall_y_ref, plan_right_ref, width)
    ranks = left.shape[0]
    lane = lax.broadcasted_iota(jnp.int32, (ranks, LANES), 1)
    out_ref[:ranks] = jnp.where(lane < dim, left, pltpu.roll(right, dim, 1))
    extra = jnp.where(lane < 2, pltpu.roll(left, LANES - dim, 1), pltpu.roll(right, LANES - dim + 2, 1))
    for j in range(ranks // LANES):
        lines = jnp.transpose(extra[j * LANES : (j + 1) * LANES])
        out_ref[ranks + 8 * j : ranks + 8 * j + 8] = lines[:8]
    used = ranks + 8 * (ranks // LANES)
    out_ref[used:] = jnp.zeros((out_ref.shape[0] - used, LANES), HIGH)


def mirror_kernel(
    sums_ref, weight_ref, plan_left_ref, plan_right_ref, mass_x_ref, mass_y_ref, flat_x_ref, flat_y_ref,
    out_ref, left_ref, right_ref, weight_out_ref, *, width, dim,
):
    ranks = plan_left_ref.shape[0]
    tiles = ranks // LANES
    lane = lax.broadcasted_iota(jnp.int32, (ranks, LANES), 1)
    lines = [sums_ref[ranks + 8 * j : ranks + 8 * j + 8] for j in range(tiles)]
    square_left, column_left, square_right, column_right = [
        jnp.concatenate([x[j : j + 1] for x in lines], axis=0) for j in range(4)
    ]
    weights = cube_root(weight_ref[...] * column_left * column_right)
    inverse_left, inverse_right = 1.0 / column_left, 1.0 / column_right
    grad_r, grad_q = square_left * inverse_left, square_right * inverse_right

    def centred(rows):
        return rows - jnp.sum(rows, keepdims=True) * (1.0 / ranks)

    def parts_of(shift):
        shift = shift * (-step_size * LOG2_E)
        high = shift.astype(HALF).astype(HIGH)
        low = (shift - high).astype(HALF).astype(HIGH)
        return high, low, shift - high - low

    def columns(first, second):
        def group(rows, j):
            empty = jnp.zeros((dim - len(rows), LANES), HIGH)
            return [x[j : j + 1] for x in rows] + [empty]

        return jnp.concatenate(
            [jnp.transpose(jnp.concatenate(group(first, j) + group(second, j), axis=0)) for j in range(tiles)],
            axis=0,
        )

    extra = columns(
        (inverse_left, inverse_right, weights * inverse_left, weights * inverse_right), parts_of(centred(grad_q))
    )
    extra_right = columns((), parts_of(centred(grad_r)))
    mean = sums_ref[:ranks] * jnp.where(lane < dim, extra[:, 0:1], extra[:, 1:2])
    swapped = pltpu.roll(mean, dim, 1)
    cross = jnp.broadcast_to(jnp.sum(mean * swapped, axis=1, keepdims=True), (ranks, LANES))
    cross = jnp.concatenate(
        [jnp.transpose(cross[j * LANES : (j + 1) * LANES])[:1] for j in range(tiles)], axis=0
    )
    weight_out_ref[...] = weights * jnp.exp(-step_size * centred(cross - grad_r - grad_q))

    def fields(points, shift, flat_ref, kernel_ref):
        points = points * (2.0 * step_size * LOG2_E)
        high = points.astype(HALF)
        rest = jnp.where(lane < dim, points - high.astype(HIGH), shift).astype(HALF)
        points = jnp.concatenate([high, rest], axis=1)
        for start in range(0, kernel_ref.shape[1], width):
            part = pl.ds(start, width)
            kernel_ref[:, part] = jnp.dot(points, flat_ref[:, part], preferred_element_type=HIGH)

    def advance(factor, plan_ref, mass_ref, kernel_ref):
        factor = jnp.broadcast_to(factor, (ranks, LANES))
        sums = []
        for start in range(0, kernel_ref.shape[1], LANES):
            part = pl.ds(start, LANES)
            kernel = plan_ref[:, part] * factor * jnp.exp2(kernel_ref[:, part])
            kernel_ref[:, part] = kernel
            sums.append(mass_ref[:, part] / jnp.sum(kernel, axis=0, keepdims=True))
        return jnp.concatenate(sums, axis=1)

    fields(jnp.where(lane < dim, swapped, mean), extra, flat_x_ref, left_ref)
    fields(jnp.where(lane < dim, mean, swapped), extra_right, flat_y_ref, right_ref)
    left = advance(extra[:, 2:3], plan_left_ref, mass_x_ref, left_ref)
    right = advance(extra[:, 3:4], plan_right_ref, mass_y_ref, right_ref)
    send(out_ref, column_sums(left_ref, left), column_sums(right_ref, right))


def combine_kernel(parts_ref, out_ref):
    out_ref[...] = jnp.broadcast_to(jnp.sum(parts_ref[...], axis=0, keepdims=True), out_ref.shape)


def last_kernel(
    parts_ref, weight_ref, scale_ref, left_ref, right_ref, point_x_ref, point_y_ref,
    left_hbm, right_hbm, weight_out_ref, left_out, right_out, sems, *, count, height,
):
    ranks = left_ref.shape[0]
    weights, scale_left, scale_right, _ = receive(parts_ref, weight_ref, scale_ref, count)
    copies = []
    for scale, point_ref, kernel_ref, buffer, target in (
        (scale_left, point_x_ref, left_ref, left_out, left_hbm),
        (scale_right, point_y_ref, right_ref, right_out, right_hbm),
    ):
        column = to_columns(scale) * float(RANK)
        for start in range(0, ranks, height):
            part = pl.ds(start, height)
            factor = wide(column[start : start + height], kernel_ref.shape[1])
            buffer[part] = point_ref[...] * kernel_ref[part] * factor
            copies.append(pltpu.make_async_copy(buffer.at[part], target.at[part], sems.at[len(copies)]))
            copies[-1].start()
    weight_out_ref[...] = weights * (RANK / count)
    for copy in copies:
        copy.wait()


def kernel_shards(cloud_x, cloud_y, mass_x, mass_y, left_start, right_start, weight_start):
    ranks, points = left_start.shape
    dim = cloud_x.shape[0]
    devices = lax.axis_size("dp")
    count = float(points * devices)
    tiles = ranks // LANES
    shape = jax.ShapeDtypeStruct
    small = shape((devices, 2 * tiles, LANES), HIGH)
    scale = shape((2 * tiles, LANES), HIGH)
    weight_shape = shape((tiles, LANES), HIGH)
    line = shape((1, points), HIGH)
    matrix = shape((ranks, points), HIGH)
    lines = -(-(ranks + 8 * tiles) // devices) * devices
    step_width = 512
    width = 256
    height = LANES // 4
    vmem_bytes = 16 * 1024 * 1024

    def call(body, out, *operands, flops, far_in=0, far_out=0, scratch=(), flags=None):
        near, far = pl.BlockSpec(memory_space=pltpu.VMEM), pl.BlockSpec(memory_space=pltpu.HBM)
        spaces = [far] * far_out + [near] * (len(out) - far_out)
        return pl.pallas_call(
            body,
            out_shape=out,
            in_specs=[far] * far_in + [near] * (len(operands) - far_in),
            out_specs=spaces,
            scratch_shapes=scratch,
            compiler_params=pltpu.CompilerParams(vmem_limit_bytes=vmem_bytes, flags=flags),
            cost_estimate=pl.CostEstimate(flops=flops, bytes_accessed=0, transcendentals=0),
        )(*[pltpu.with_memory_space_constraint(x, pltpu.HBM) for x in operands[:far_in]], *operands[far_in:])

    def exchange(sent):
        return lax.all_to_all(sent, "dp", 0, 0)

    step_flops = 8 * ranks * points
    mass_x, mass_y = mass_x.reshape(1, points), mass_y.reshape(1, points)
    weight = weight_start.reshape(tiles, LANES)
    cloud_shapes = (shape((points, 2 * LANES), HALF), shape((4 * dim, points), HALF))
    parts, left, right, mass_x, mass_y, tall_x, flat_x, tall_y, flat_y = call(
        functools.partial(first_kernel, width=step_width),
        (small, matrix, matrix, line, line, *cloud_shapes, *cloud_shapes),
        left_start, right_start, mass_x, mass_y, cloud_x, cloud_y,
        flops=step_flops,
        far_in=6,
        scratch=[
            pltpu.VMEM(cloud_x.shape, HIGH),
            pltpu.VMEM(cloud_y.shape, HIGH),
            pltpu.SemaphoreType.DMA((2 + 2 * points // step_width,)),
            pltpu.SemaphoreType.DMA((2,)),
        ],
    )
    for outer in range(MIRROR + 1):
        scaling = ()
        for repeat in range(1, INNER):
            parts = exchange(parts)
            if repeat == INNER - 1 and outer < MIRROR:
                break
            first = outer == 0 and repeat == 1
            keep = outer == MIRROR and repeat == INNER - 1
            body = functools.partial(
                step_kernel, count=count, first=first, fresh=repeat == 1, keep=keep
            )
            out = (small, scale) + (line, line) * (first + keep)
            parts, new_scaling, *more = call(
                body, out, parts, weight, *scaling, left, right, mass_x, mass_y, flops=step_flops
            )
            scaling = (new_scaling,)
            if first:
                mass_x, mass_y = more
        if outer == MIRROR:
            break
        sent, left, right = call(
            functools.partial(moment_kernel, width=width, count=count, dim=dim),
            (shape((lines, LANES), HIGH), matrix, matrix),
            parts, weight, *scaling, left, right, mass_x, mass_y, tall_x, tall_y,
            flops=step_flops + 16 * ranks * points * LANES,
        )
        sent = exchange(sent.reshape(devices, 1, -1))
        (sent,) = call(combine_kernel, (shape(sent.shape, HIGH),), sent, flops=lines * LANES)
        sums = exchange(sent).reshape(lines, LANES)
        parts, left, right, weight = call(
            functools.partial(mirror_kernel, width=width, dim=dim),
            (small, matrix, matrix, weight_shape),
            sums, weight, left, right, mass_x, mass_y, flat_x, flat_y,
            flops=step_flops + 16 * ranks * points * dim,
        )
    parts = exchange(parts)
    left, right, weights = call(
        functools.partial(last_kernel, count=count, height=height),
        (matrix, matrix, weight_shape),
        parts, weight, *scaling, left, right, *more,
        flops=step_flops,
        far_out=2,
        scratch=[
            pltpu.VMEM((ranks, points), HIGH),
            pltpu.VMEM((ranks, points), HIGH),
            pltpu.SemaphoreType.DMA((2 * ranks // height,)),
        ],
    )
    return (left, right, weights.reshape(ranks))


def device_program(cloud_x, cloud_y, mass_x, mass_y, left_start, right_start, weight_start):
    ranks, points = left_start.shape
    whole = lax.axis_size("rank") == 1 and cloud_x.shape[0] == LANES // 2
    body = kernel_shards if whole and ranks % LANES == 0 and points % 512 == 0 else shards
    return body(cloud_x, cloud_y, mass_x, mass_y, left_start, right_start, weight_start)


def solution(mesh):
    in_specs = (
        P(None, "dp"),
        P(None, "dp"),
        P("dp"),
        P("dp"),
        P("rank", "dp"),
        P("rank", "dp"),
        P("rank"),
    )
    out_specs = (P("rank", "dp"), P("rank", "dp"), P("rank"))
    return jax.shard_map(device_program, mesh=mesh, in_specs=in_specs, out_specs=out_specs, check_vma=False)
```

```python
import functools

import jax
import jax.numpy as jnp
from jax import lax
from jax.experimental import pallas as pl
from jax.experimental.pallas import tpu as pltpu
from jax.sharding import PartitionSpec as P

RANK = 256
INNER = 4
MIRROR = 3


exact_mode = lax.Precision.HIGHEST
step_size = 2.0


def total_small(part):
    count = lax.axis_size("dp")
    parts = lax.all_to_all(jnp.broadcast_to(part[None], (count,) + part.shape), "dp", 0, 0)
    return jnp.sum(parts, axis=0)


def total_large(part):
    count = lax.axis_size("dp")
    size = part.shape[0]
    piece = -(-size // (count * 128)) * 128
    padded = jnp.pad(part, (0, piece * count - size)).reshape(count, 1, piece)
    mine = jnp.sum(lax.all_to_all(padded, "dp", 0, 0), axis=0)
    parts = lax.all_to_all(jnp.broadcast_to(mine[None], (count, 1, piece)), "dp", 0, 0)
    return parts.reshape(-1)[:size]


def over_rank(value):
    return lax.psum(value, "rank") if lax.axis_size("rank") > 1 else value


def shards(cloud_x, cloud_y, mass_x, mass_y, left_start, right_start, weight_start):
    ranks_local = left_start.shape[0]
    points_dev = left_start.shape[1]
    dim = cloud_x.shape[0]
    total_count = float(points_dev * lax.axis_size("dp"))
    square_x = jnp.sum(cloud_x * cloud_x, axis=0)
    square_y = jnp.sum(cloud_y * cloud_y, axis=0)

    def rows(scale, kernel):
        return over_rank(jnp.sum(scale[:, None] * kernel, axis=0))

    def columns(kernel, point):
        return jnp.sum(kernel * point[None, :], axis=1)

    left_mass, right_mass = mass_x, mass_y
    kernel_left, kernel_right, kernel_weight = left_start, right_start, weight_start
    for outer in range(MIRROR + 1):
        scale_left = jnp.ones((ranks_local,), jnp.float32)
        scale_right = jnp.ones((ranks_local,), jnp.float32)
        for repeat in range(INNER):
            point_left = left_mass / rows(scale_left, kernel_left)
            point_right = right_mass / rows(scale_right, kernel_right)
            if repeat == INNER - 1 and outer < MIRROR:
                break
            column_left = columns(kernel_left, point_left)
            column_right = columns(kernel_right, point_right)
            if outer == 0 and repeat == 0:
                sums = jnp.stack([jnp.sum(mass_x), jnp.sum(mass_y)])
                packed = total_small(jnp.concatenate([column_left, column_right, sums])[None])[0]
                factor_x = total_count / packed[2 * ranks_local]
                factor_y = total_count / packed[2 * ranks_local + 1]
                left_mass = mass_x * factor_x
                right_mass = mass_y * factor_y
                column_left = packed[:ranks_local] * factor_x
                column_right = packed[ranks_local : 2 * ranks_local] * factor_y
            else:
                packed = total_small(jnp.concatenate([column_left, column_right])[None])[0]
                column_left = packed[:ranks_local]
                column_right = packed[ranks_local:]
            weights = jnp.cbrt(
                kernel_weight * scale_left * column_left * scale_right * column_right
            )
            scale_left = weights / column_left
            scale_right = weights / column_right
        if outer == MIRROR:
            break
        plan_left = kernel_left * point_left[None, :] * scale_left[:, None]
        plan_right = kernel_right * point_right[None, :] * scale_right[:, None]
        packed = total_large(
            jnp.concatenate(
                [
                    jnp.dot(cloud_x, plan_left.T, precision=exact_mode).reshape(-1),
                    jnp.dot(cloud_y, plan_right.T, precision=exact_mode).reshape(-1),
                    jnp.sum(plan_left * square_x[None, :], axis=1),
                    jnp.sum(plan_right * square_y[None, :], axis=1),
                    jnp.sum(plan_left, axis=1),
                    jnp.sum(plan_right, axis=1),
                ]
            )
        )
        packed = packed.reshape(2 * dim + 4, ranks_local)
        column_left, column_right = packed[2 * dim + 2], packed[2 * dim + 3]
        weights = jnp.cbrt(kernel_weight * column_left * column_right)
        mean_x = packed[:dim] / column_left
        mean_y = packed[dim : 2 * dim] / column_right
        grad_q = packed[2 * dim + 1] / column_right
        grad_r = packed[2 * dim] / column_left
        grad_g = -(grad_r + grad_q - 2.0 * jnp.sum(mean_x * mean_y, axis=0))
        centre = over_rank(jnp.stack([jnp.sum(grad_q), jnp.sum(grad_r), jnp.sum(grad_g)])) / RANK
        field_q = (grad_q - centre[0])[:, None] - 2.0 * jnp.dot(mean_y.T, cloud_x, precision=exact_mode)
        field_r = (grad_r - centre[1])[:, None] - 2.0 * jnp.dot(mean_x.T, cloud_y, precision=exact_mode)
        kernel_left = plan_left * (weights / column_left)[:, None] * jnp.exp(-step_size * field_q)
        kernel_right = plan_right * (weights / column_right)[:, None] * jnp.exp(-step_size * field_r)
        kernel_weight = weights * jnp.exp(-step_size * (grad_g - centre[2]))
    left = point_left[None, :] * kernel_left * scale_left[:, None]
    right = point_right[None, :] * kernel_right * scale_right[:, None]
    return (RANK * left, RANK * right, weights * (RANK / total_count))


LANES = 128
HIGH = jnp.float32
HALF = jnp.bfloat16
LOG2_E = 1.4426950408889634
STATS = 8


def halves(value):
    high = value.astype(HALF)
    return high, (value - high.astype(HIGH)).astype(HALF)


def cube_root(value):
    inverse = jnp.exp2(jnp.log2(value) * (-1.0 / 3.0))
    scaled = value * inverse
    inverse = inverse + inverse * (1.0 - scaled * inverse * inverse) * (1.0 / 3.0)
    return value * inverse * inverse


def tree_sum(ref):
    parts = [ref[j] for j in range(ref.shape[0])]
    while len(parts) > 1:
        pairs = [parts[j] + parts[j + 1] for j in range(0, len(parts) - 1, 2)]
        parts = pairs + parts[len(parts) - len(parts) % 2 :]
    return parts[0]


def to_columns(rows):
    return jnp.concatenate(
        [jnp.transpose(jnp.broadcast_to(rows[j : j + 1], (LANES, LANES))) for j in range(rows.shape[0])],
        axis=0,
    )


def to_rows(block):
    return jnp.concatenate(
        [
            jnp.sum(jnp.transpose(block[j : j + LANES]), axis=0, keepdims=True)
            for j in range(0, block.shape[0], LANES)
        ],
        axis=0,
    )


def wide(column, width):
    return jnp.concatenate([column] * (width // LANES), axis=1)


def fold(block):
    total = block[:, :LANES]
    for j in range(LANES, block.shape[1], LANES):
        total = total + block[:, j : j + LANES]
    return total


def points_of(kernel_ref, column, mass_ref):
    points = []
    for start in range(0, kernel_ref.shape[1], LANES):
        part = pl.ds(start, LANES)
        block = kernel_ref[:, part]
        if column is not None:
            block = block * column
        points.append(mass_ref[:, part] / jnp.sum(block, axis=0, keepdims=True))
    return jnp.concatenate(points, axis=1)


def column_sums(kernel_ref, point):
    spread = jnp.broadcast_to(point, (8, point.shape[1]))
    return jnp.concatenate(
        [fold(kernel_ref[pl.ds(row, 8), :] * spread) for row in range(0, kernel_ref.shape[0], 8)], axis=0
    )


def send(out_ref, left, right):
    packed = jnp.concatenate([to_rows(left), to_rows(right)], axis=0)
    out_ref[...] = jnp.broadcast_to(packed[None], out_ref.shape)


def receive(parts_ref, weight_ref, scale_ref, count):
    rows = weight_ref.shape[0]
    totals = tree_sum(parts_ref)
    column_left, column_right = totals[:rows], totals[rows:]
    factors = None
    if scale_ref is None:
        factors = [count / jnp.sum(c, keepdims=True) for c in (column_left, column_right)]
        column_left = column_left * factors[0]
        column_right = column_right * factors[1]
        weights = cube_root(weight_ref[...] * column_left * column_right)
    else:
        weights = cube_root(
            weight_ref[...] * scale_ref[:rows] * column_left * scale_ref[rows:] * column_right
        )
    return weights, weights / column_left, weights / column_right, factors


def first_kernel(
    left_hbm, right_hbm, mass_x_hbm, mass_y_hbm, out_ref, left_ref, right_ref, mass_x_ref, mass_y_ref, sems, *, width
):
    points = left_ref.shape[1]
    small = [
        pltpu.make_async_copy(mass_x_hbm, mass_x_ref, sems.at[0]),
        pltpu.make_async_copy(mass_y_hbm, mass_y_ref, sems.at[1]),
    ]
    large = []
    for source, target in ((left_hbm, left_ref), (right_hbm, right_ref)):
        for start in range(0, points, width):
            part = pl.ds(start, width)
            sem = sems.at[2 + len(large)]
            large.append(pltpu.make_async_copy(source.at[:, part], target.at[:, part], sem))
    for copy in small + large:
        copy.start()
    for copy in small:
        copy.wait()
    half = len(large) // 2
    sums = []
    for kernel_ref, mass_ref, copies in (
        (left_ref, mass_x_ref, large[:half]),
        (right_ref, mass_y_ref, large[half:]),
    ):
        total = None
        for start, copy in zip(range(0, points, width), copies):
            copy.wait()
            part = pl.ds(start, width)
            block = kernel_ref.at[:, part]
            piece = column_sums(block, points_of(block, None, mass_ref.at[:, part]))
            total = piece if total is None else total + piece
        sums.append(total)
    send(out_ref, *sums)


def step_kernel(*refs, count, first, fresh, keep):
    refs = list(refs)
    if first:
        cloud_x_ref, cloud_y_ref = refs[:2]
        del refs[:2]
    parts_ref, weight_ref = refs[:2]
    del refs[:2]
    scale_in = None if fresh else refs.pop(0)
    left_ref, right_ref, mass_x_ref, mass_y_ref, out_ref, scale_ref = refs[:6]
    del refs[:6]
    if fresh and not first:
        rows = weight_ref.shape[0]
        totals = tree_sum(parts_ref)
        weights = cube_root(weight_ref[...] * totals[:rows] * totals[rows:])
        scale_left, scale_right, factors = weights / totals[:rows], weights / totals[rows:], None
    else:
        _, scale_left, scale_right, factors = receive(parts_ref, weight_ref, scale_in, count)
    scale_ref[...] = jnp.concatenate([scale_left, scale_right], axis=0)
    if first:
        new_x_ref, new_y_ref = refs[:2]
        del refs[:2]
        new_x_ref[...] = mass_x_ref[...] * factors[0]
        new_y_ref[...] = mass_y_ref[...] * factors[1]
        mass_x_ref, mass_y_ref = new_x_ref, new_y_ref
    point_x_ref, point_y_ref = refs[:2] if keep else (None, None)
    point_x = points_of(left_ref, to_columns(scale_left), mass_x_ref)
    point_y = points_of(right_ref, to_columns(scale_right), mass_y_ref)
    send(out_ref, column_sums(left_ref, point_x), column_sums(right_ref, point_y))
    if keep:
        point_x_ref[...] = point_x
        point_y_ref[...] = point_y
    if first:
        halve_cloud(cloud_x_ref, refs[0], refs[1], 0)
        halve_cloud(cloud_y_ref, refs[2], refs[3], STATS)


def halve_cloud(cloud_ref, tall_ref, flat_ref, place):
    dim, width = cloud_ref.shape[0], 4 * LANES
    lines = lax.broadcasted_iota(jnp.int32, (2 * STATS, width), 0) - place
    ones = jnp.where(lax.broadcasted_iota(jnp.int32, (dim, width), 0) < 3, 1.0, 0.0).astype(HALF)
    for start in range(0, cloud_ref.shape[1], width):
        part = pl.ds(start, width)
        points = cloud_ref[:, part]
        high, low = halves(points)
        square = jnp.sum(points * points, axis=0, keepdims=True)
        square_high = square.astype(HALF).astype(HIGH)
        stats = jnp.where(lines == 1, square - square_high, jnp.where(lines == 2, 1.0, 0.0))
        stats = jnp.where(lines == 0, square_high, stats).astype(HALF)
        tall_ref[:, part] = jnp.concatenate([high, low, stats], axis=0)
        flat_ref[:, part] = jnp.concatenate([high, low, high, ones], axis=0)


def moment_side(kernel_ref, column, mass_ref, tall_ref, plan_ref, width):
    total = None
    for start in range(0, kernel_ref.shape[1], width):
        part = pl.ds(start, width)
        scaled = kernel_ref[:, part] * wide(column, width)
        plan = scaled * (mass_ref[:, part] / jnp.sum(scaled, axis=0, keepdims=True))
        plan_ref[:, part] = plan
        high, low = halves(plan)
        tall = tall_ref[:, part]
        piece = lax.dot_general(high, tall, (((1,), (1,)), ((), ())), preferred_element_type=HIGH)
        piece = piece + lax.dot_general(low, tall, (((1,), (1,)), ((), ())), preferred_element_type=HIGH)
        total = piece if total is None else total + piece
    return total


def moment_kernel(
    parts_ref, weight_ref, scale_ref, left_ref, right_ref, mass_x_ref, mass_y_ref, tall_x_ref, tall_y_ref,
    out_ref, plan_left_ref, plan_right_ref, *, width, count, dim,
):
    _, scale_left, scale_right, _ = receive(parts_ref, weight_ref, scale_ref, count)
    left = moment_side(left_ref, to_columns(scale_left), mass_x_ref, tall_x_ref, plan_left_ref, width)
    right = moment_side(right_ref, to_columns(scale_right), mass_y_ref, tall_y_ref, plan_right_ref, width)
    ranks = left.shape[0]
    lane = lax.broadcasted_iota(jnp.int32, (ranks, LANES), 1)
    products = [x[:, :LANES] + pltpu.roll(x[:, :LANES], dim, 1) for x in (left, right)]
    out_ref[:ranks] = jnp.where(lane < dim, *products)
    extra = jnp.concatenate(
        [left[:, LANES:] + right[:, LANES:], jnp.zeros((ranks, LANES - 2 * STATS), HIGH)], axis=1
    )
    used = ranks
    for j in range(0, ranks, LANES):
        out_ref[used : used + 2 * STATS] = jnp.transpose(extra[j : j + LANES])[: 2 * STATS]
        used += 2 * STATS
    if used < out_ref.shape[0]:
        out_ref[used:] = jnp.zeros((out_ref.shape[0] - used, LANES), HIGH)


def mirror_kernel(
    sums_ref, weight_ref, plan_left_ref, plan_right_ref, mass_x_ref, mass_y_ref, flat_x_ref, flat_y_ref,
    out_ref, left_ref, right_ref, weight_out_ref, *, width, dim,
):
    ranks = plan_left_ref.shape[0]
    tiles = ranks // LANES
    lane = lax.broadcasted_iota(jnp.int32, (ranks, LANES), 1)
    lines = [sums_ref[ranks + 2 * STATS * j : ranks + 2 * STATS * (j + 1)] for j in range(tiles)]

    def line(j):
        return jnp.concatenate([x[j : j + 1] for x in lines], axis=0)

    square_left, column_left = line(0) + line(1), line(2)
    square_right, column_right = line(STATS) + line(STATS + 1), line(STATS + 2)
    weights = cube_root(weight_ref[...] * column_left * column_right)
    inverse_left, inverse_right = 1.0 / column_left, 1.0 / column_right
    grad_r, grad_q = square_left * inverse_left, square_right * inverse_right

    def centred(rows):
        return rows - jnp.sum(rows, keepdims=True) * (1.0 / ranks)

    def parts_of(shift):
        shift = shift * (-step_size * LOG2_E)
        high = shift.astype(HALF).astype(HIGH)
        low = (shift - high).astype(HALF).astype(HIGH)
        return high, low, shift - high - low

    def columns(first, second):
        def group(rows, j):
            empty = jnp.zeros((dim - len(rows), LANES), HIGH)
            return [x[j : j + 1] for x in rows] + [empty]

        return jnp.concatenate(
            [jnp.transpose(jnp.concatenate(group(first, j) + group(second, j), axis=0)) for j in range(tiles)],
            axis=0,
        )

    extra = columns(
        (inverse_left, inverse_right, weights * inverse_left, weights * inverse_right), parts_of(centred(grad_q))
    )
    extra_right = columns((), parts_of(centred(grad_r)))
    mean = sums_ref[:ranks] * jnp.where(lane < dim, extra[:, 0:1], extra[:, 1:2])
    swapped = pltpu.roll(mean, dim, 1)
    cross = jnp.broadcast_to(jnp.sum(mean * swapped, axis=1, keepdims=True), (ranks, LANES))
    cross = jnp.concatenate(
        [jnp.transpose(cross[j * LANES : (j + 1) * LANES])[:1] for j in range(tiles)], axis=0
    )
    weight_out_ref[...] = weights * jnp.exp(-step_size * centred(cross - grad_r - grad_q))

    def fields(points, shift, flat_ref, kernel_ref):
        points = points * (2.0 * step_size * LOG2_E)
        high = points.astype(HALF)
        rest = jnp.where(lane < dim, points - high.astype(HIGH), shift).astype(HALF)
        points = jnp.concatenate([high, rest], axis=1)
        for start in range(0, kernel_ref.shape[1], width):
            part = pl.ds(start, width)
            kernel_ref[:, part] = jnp.dot(points, flat_ref[:, part], preferred_element_type=HIGH)

    def advance(factor, plan_ref, mass_ref, kernel_ref):
        factor = jnp.broadcast_to(factor, (ranks, LANES))
        sums = []
        for start in range(0, kernel_ref.shape[1], LANES):
            part = pl.ds(start, LANES)
            kernel = plan_ref[:, part] * factor * jnp.exp2(kernel_ref[:, part])
            kernel_ref[:, part] = kernel
            sums.append(mass_ref[:, part] / jnp.sum(kernel, axis=0, keepdims=True))
        return jnp.concatenate(sums, axis=1)

    fields(jnp.where(lane < dim, swapped, mean), extra, flat_x_ref, left_ref)
    fields(jnp.where(lane < dim, mean, swapped), extra_right, flat_y_ref, right_ref)
    left = advance(extra[:, 2:3], plan_left_ref, mass_x_ref, left_ref)
    right = advance(extra[:, 3:4], plan_right_ref, mass_y_ref, right_ref)
    send(out_ref, column_sums(left_ref, left), column_sums(right_ref, right))


def combine_kernel(parts_ref, out_ref):
    out_ref[...] = jnp.broadcast_to(jnp.sum(parts_ref[...], axis=0, keepdims=True), out_ref.shape)


def last_kernel(
    parts_ref, weight_ref, scale_ref, left_ref, right_ref, point_x_ref, point_y_ref,
    left_hbm, right_hbm, weight_out_ref, left_out, right_out, sems, *, count, height,
):
    ranks = left_ref.shape[0]
    weights, scale_left, scale_right, _ = receive(parts_ref, weight_ref, scale_ref, count)
    copies = []
    for scale, point_ref, kernel_ref, buffer, target in (
        (scale_left, point_x_ref, left_ref, left_out, left_hbm),
        (scale_right, point_y_ref, right_ref, right_out, right_hbm),
    ):
        column = to_columns(scale) * float(RANK)
        for start in range(0, ranks, height):
            part = pl.ds(start, height)
            factor = wide(column[start : start + height], kernel_ref.shape[1])
            buffer[part] = point_ref[...] * kernel_ref[part] * factor
            copies.append(pltpu.make_async_copy(buffer.at[part], target.at[part], sems.at[len(copies)]))
            copies[-1].start()
    weight_out_ref[...] = weights * (RANK / count)
    for copy in copies:
        copy.wait()


def kernel_shards(cloud_x, cloud_y, mass_x, mass_y, left_start, right_start, weight_start):
    ranks, points = left_start.shape
    dim = cloud_x.shape[0]
    devices = lax.axis_size("dp")
    count = float(points * devices)
    tiles = ranks // LANES
    shape = jax.ShapeDtypeStruct
    small = shape((devices, 2 * tiles, LANES), HIGH)
    scale = shape((2 * tiles, LANES), HIGH)
    weight_shape = shape((tiles, LANES), HIGH)
    line = shape((1, points), HIGH)
    matrix = shape((ranks, points), HIGH)
    lines = -(-(ranks + 2 * STATS * tiles) // devices) * devices
    step_width = 512
    width = 256
    height = LANES // 4
    vmem_bytes = 16 * 1024 * 1024

    def call(body, out, *operands, flops, far_in=0, far_out=0, scratch=(), flags=None):
        near, far = pl.BlockSpec(memory_space=pltpu.VMEM), pl.BlockSpec(memory_space=pltpu.HBM)
        spaces = [far] * far_out + [near] * (len(out) - far_out)
        return pl.pallas_call(
            body,
            out_shape=out,
            in_specs=[far] * far_in + [near] * (len(operands) - far_in),
            out_specs=spaces,
            scratch_shapes=scratch,
            compiler_params=pltpu.CompilerParams(vmem_limit_bytes=vmem_bytes, flags=flags),
            cost_estimate=pl.CostEstimate(flops=flops, bytes_accessed=0, transcendentals=0),
        )(*[pltpu.with_memory_space_constraint(x, pltpu.HBM) for x in operands[:far_in]], *operands[far_in:])

    def exchange(sent):
        return lax.all_to_all(sent, "dp", 0, 0)

    step_flops = 8 * ranks * points
    mass_x, mass_y = mass_x.reshape(1, points), mass_y.reshape(1, points)
    weight = weight_start.reshape(tiles, LANES)
    cloud_shapes = (shape((2 * dim + 2 * STATS, points), HALF), shape((4 * dim, points), HALF))
    parts, left, right, mass_x, mass_y = call(
        functools.partial(first_kernel, width=step_width),
        (small, matrix, matrix, line, line),
        left_start, right_start, mass_x, mass_y,
        flops=step_flops,
        far_in=4,
        scratch=[pltpu.SemaphoreType.DMA((2 + 2 * points // step_width,))],
    )
    for outer in range(MIRROR + 1):
        scaling = ()
        for repeat in range(1, INNER):
            parts = exchange(parts)
            if repeat == INNER - 1 and outer < MIRROR:
                break
            first = outer == 0 and repeat == 1
            keep = outer == MIRROR and repeat == INNER - 1
            body = functools.partial(
                step_kernel, count=count, first=first, fresh=repeat == 1, keep=keep
            )
            out = (small, scale) + (line, line) * (first + keep) + cloud_shapes * (2 * first)
            clouds = (cloud_x, cloud_y) * first
            parts, new_scaling, *more = call(
                body, out, *clouds, parts, weight, *scaling, left, right, mass_x, mass_y, flops=step_flops
            )
            scaling = (new_scaling,)
            if first:
                mass_x, mass_y, tall_x, flat_x, tall_y, flat_y = more
        if outer == MIRROR:
            break
        sent, left, right = call(
            functools.partial(moment_kernel, width=width, count=count, dim=dim),
            (shape((lines, LANES), HIGH), matrix, matrix),
            parts, weight, *scaling, left, right, mass_x, mass_y, tall_x, tall_y,
            flops=step_flops + 16 * ranks * points * LANES,
        )
        sent = exchange(sent.reshape(devices, 1, -1))
        (sent,) = call(combine_kernel, (shape(sent.shape, HIGH),), sent, flops=lines * LANES)
        sums = exchange(sent).reshape(lines, LANES)
        parts, left, right, weight = call(
            functools.partial(mirror_kernel, width=width, dim=dim),
            (small, matrix, matrix, weight_shape),
            sums, weight, left, right, mass_x, mass_y, flat_x, flat_y,
            flops=step_flops + 16 * ranks * points * dim,
        )
    parts = exchange(parts)
    left, right, weights = call(
        functools.partial(last_kernel, count=count, height=height),
        (matrix, matrix, weight_shape),
        parts, weight, *scaling, left, right, *more,
        flops=step_flops,
        far_out=2,
        scratch=[
            pltpu.VMEM((ranks, points), HIGH),
            pltpu.VMEM((ranks, points), HIGH),
            pltpu.SemaphoreType.DMA((2 * ranks // height,)),
        ],
    )
    return (left, right, weights.reshape(ranks))


def device_program(cloud_x, cloud_y, mass_x, mass_y, left_start, right_start, weight_start):
    ranks, points = left_start.shape
    whole = lax.axis_size("rank") == 1 and cloud_x.shape[0] == LANES // 2
    body = kernel_shards if whole and ranks % LANES == 0 and points % 512 == 0 else shards
    return body(cloud_x, cloud_y, mass_x, mass_y, left_start, right_start, weight_start)


def solution(mesh):
    in_specs = (
        P(None, "dp"),
        P(None, "dp"),
        P("dp"),
        P("dp"),
        P("rank", "dp"),
        P("rank", "dp"),
        P("rank"),
    )
    out_specs = (P("rank", "dp"), P("rank", "dp"), P("rank"))
    return jax.shard_map(device_program, mesh=mesh, in_specs=in_specs, out_specs=out_specs, check_vma=False)
```

```python
import functools

import jax
import jax.numpy as jnp
from jax import lax
from jax.experimental import pallas as pl
from jax.experimental.pallas import tpu as pltpu
from jax.sharding import PartitionSpec as P

RANK = 256
INNER = 4
MIRROR = 3


exact_mode = lax.Precision.HIGHEST
step_size = 2.0


def total_small(part):
    count = lax.axis_size("dp")
    parts = lax.all_to_all(jnp.broadcast_to(part[None], (count,) + part.shape), "dp", 0, 0)
    return jnp.sum(parts, axis=0)


def total_large(part):
    count = lax.axis_size("dp")
    size = part.shape[0]
    piece = -(-size // (count * 128)) * 128
    padded = jnp.pad(part, (0, piece * count - size)).reshape(count, 1, piece)
    mine = jnp.sum(lax.all_to_all(padded, "dp", 0, 0), axis=0)
    parts = lax.all_to_all(jnp.broadcast_to(mine[None], (count, 1, piece)), "dp", 0, 0)
    return parts.reshape(-1)[:size]


def over_rank(value):
    return lax.psum(value, "rank") if lax.axis_size("rank") > 1 else value


def shards(cloud_x, cloud_y, mass_x, mass_y, left_start, right_start, weight_start):
    ranks_local = left_start.shape[0]
    points_dev = left_start.shape[1]
    dim = cloud_x.shape[0]
    total_count = float(points_dev * lax.axis_size("dp"))
    square_x = jnp.sum(cloud_x * cloud_x, axis=0)
    square_y = jnp.sum(cloud_y * cloud_y, axis=0)

    def rows(scale, kernel):
        return over_rank(jnp.sum(scale[:, None] * kernel, axis=0))

    def columns(kernel, point):
        return jnp.sum(kernel * point[None, :], axis=1)

    left_mass, right_mass = mass_x, mass_y
    kernel_left, kernel_right, kernel_weight = left_start, right_start, weight_start
    for outer in range(MIRROR + 1):
        scale_left = jnp.ones((ranks_local,), jnp.float32)
        scale_right = jnp.ones((ranks_local,), jnp.float32)
        for repeat in range(INNER):
            point_left = left_mass / rows(scale_left, kernel_left)
            point_right = right_mass / rows(scale_right, kernel_right)
            if repeat == INNER - 1 and outer < MIRROR:
                break
            column_left = columns(kernel_left, point_left)
            column_right = columns(kernel_right, point_right)
            if outer == 0 and repeat == 0:
                sums = jnp.stack([jnp.sum(mass_x), jnp.sum(mass_y)])
                packed = total_small(jnp.concatenate([column_left, column_right, sums])[None])[0]
                factor_x = total_count / packed[2 * ranks_local]
                factor_y = total_count / packed[2 * ranks_local + 1]
                left_mass = mass_x * factor_x
                right_mass = mass_y * factor_y
                column_left = packed[:ranks_local] * factor_x
                column_right = packed[ranks_local : 2 * ranks_local] * factor_y
            else:
                packed = total_small(jnp.concatenate([column_left, column_right])[None])[0]
                column_left = packed[:ranks_local]
                column_right = packed[ranks_local:]
            weights = jnp.cbrt(
                kernel_weight * scale_left * column_left * scale_right * column_right
            )
            scale_left = weights / column_left
            scale_right = weights / column_right
        if outer == MIRROR:
            break
        plan_left = kernel_left * point_left[None, :] * scale_left[:, None]
        plan_right = kernel_right * point_right[None, :] * scale_right[:, None]
        packed = total_large(
            jnp.concatenate(
                [
                    jnp.dot(cloud_x, plan_left.T, precision=exact_mode).reshape(-1),
                    jnp.dot(cloud_y, plan_right.T, precision=exact_mode).reshape(-1),
                    jnp.sum(plan_left * square_x[None, :], axis=1),
                    jnp.sum(plan_right * square_y[None, :], axis=1),
                    jnp.sum(plan_left, axis=1),
                    jnp.sum(plan_right, axis=1),
                ]
            )
        )
        packed = packed.reshape(2 * dim + 4, ranks_local)
        column_left, column_right = packed[2 * dim + 2], packed[2 * dim + 3]
        weights = jnp.cbrt(kernel_weight * column_left * column_right)
        mean_x = packed[:dim] / column_left
        mean_y = packed[dim : 2 * dim] / column_right
        grad_q = packed[2 * dim + 1] / column_right
        grad_r = packed[2 * dim] / column_left
        grad_g = -(grad_r + grad_q - 2.0 * jnp.sum(mean_x * mean_y, axis=0))
        centre = over_rank(jnp.stack([jnp.sum(grad_q), jnp.sum(grad_r), jnp.sum(grad_g)])) / RANK
        field_q = (grad_q - centre[0])[:, None] - 2.0 * jnp.dot(mean_y.T, cloud_x, precision=exact_mode)
        field_r = (grad_r - centre[1])[:, None] - 2.0 * jnp.dot(mean_x.T, cloud_y, precision=exact_mode)
        kernel_left = plan_left * (weights / column_left)[:, None] * jnp.exp(-step_size * field_q)
        kernel_right = plan_right * (weights / column_right)[:, None] * jnp.exp(-step_size * field_r)
        kernel_weight = weights * jnp.exp(-step_size * (grad_g - centre[2]))
    left = point_left[None, :] * kernel_left * scale_left[:, None]
    right = point_right[None, :] * kernel_right * scale_right[:, None]
    return (RANK * left, RANK * right, weights * (RANK / total_count))


LANES = 128
HIGH = jnp.float32
HALF = jnp.bfloat16
LOG2_E = 1.4426950408889634
STATS = 8
SMALLEST = 2.0**-126


def halves(value):
    high = value.astype(HALF)
    return high, (value - high.astype(HIGH)).astype(HALF)


def cube_root(value):
    inverse = jnp.exp2(jnp.log2(value) * (-1.0 / 3.0))
    scaled = value * inverse
    inverse = inverse + inverse * (1.0 - scaled * inverse * inverse) * (1.0 / 3.0)
    return jnp.where(value < SMALLEST, 0.0, value * inverse * inverse)


def tree_sum(ref):
    parts = [ref[j] for j in range(ref.shape[0])]
    while len(parts) > 1:
        pairs = [parts[j] + parts[j + 1] for j in range(0, len(parts) - 1, 2)]
        parts = pairs + parts[len(parts) - len(parts) % 2 :]
    return parts[0]


def to_columns(rows):
    return jnp.concatenate(
        [jnp.transpose(jnp.broadcast_to(rows[j : j + 1], (LANES, LANES))) for j in range(rows.shape[0])],
        axis=0,
    )


def to_rows(block):
    return jnp.concatenate(
        [
            jnp.sum(jnp.transpose(block[j : j + LANES]), axis=0, keepdims=True)
            for j in range(0, block.shape[0], LANES)
        ],
        axis=0,
    )


def wide(column, width):
    return jnp.concatenate([column] * (width // LANES), axis=1)


def fold(block):
    total = block[:, :LANES]
    for j in range(LANES, block.shape[1], LANES):
        total = total + block[:, j : j + LANES]
    return total


def points_of(kernel_ref, column, mass_ref):
    points = []
    for start in range(0, kernel_ref.shape[1], LANES):
        part = pl.ds(start, LANES)
        block = kernel_ref[:, part]
        if column is not None:
            block = block * column
        points.append(mass_ref[:, part] / jnp.sum(block, axis=0, keepdims=True))
    return jnp.concatenate(points, axis=1)


def column_sums(kernel_ref, point):
    spread = jnp.broadcast_to(point, (8, point.shape[1]))
    return jnp.concatenate(
        [fold(kernel_ref[pl.ds(row, 8), :] * spread) for row in range(0, kernel_ref.shape[0], 8)], axis=0
    )


def send(out_ref, left, right):
    packed = jnp.concatenate([to_rows(left), to_rows(right)], axis=0)
    out_ref[...] = jnp.broadcast_to(packed[None], out_ref.shape)


def receive(parts_ref, weight_ref, scale_ref, count):
    rows = weight_ref.shape[0]
    totals = tree_sum(parts_ref)
    column_left, column_right = totals[:rows], totals[rows:]
    factors = None
    if scale_ref is None:
        factors = [count / jnp.sum(c, keepdims=True) for c in (column_left, column_right)]
        column_left = column_left * factors[0]
        column_right = column_right * factors[1]
        weights = cube_root(weight_ref[...] * column_left * column_right)
    else:
        weights = cube_root(
            weight_ref[...] * scale_ref[:rows] * column_left * scale_ref[rows:] * column_right
        )
    return weights, weights / column_left, weights / column_right, factors


def first_kernel(
    left_hbm, right_hbm, mass_x_hbm, mass_y_hbm, out_ref, left_ref, right_ref, mass_x_ref, mass_y_ref, sems, *, width
):
    points = left_ref.shape[1]
    small = [
        pltpu.make_async_copy(mass_x_hbm, mass_x_ref, sems.at[0]),
        pltpu.make_async_copy(mass_y_hbm, mass_y_ref, sems.at[1]),
    ]
    large = []
    for source, target in ((left_hbm, left_ref), (right_hbm, right_ref)):
        for start in range(0, points, width):
            part = pl.ds(start, width)
            sem = sems.at[2 + len(large)]
            large.append(pltpu.make_async_copy(source.at[:, part], target.at[:, part], sem))
    for copy in small + large:
        copy.start()
    for copy in small:
        copy.wait()
    half = len(large) // 2
    sums = []
    for kernel_ref, mass_ref, copies in (
        (left_ref, mass_x_ref, large[:half]),
        (right_ref, mass_y_ref, large[half:]),
    ):
        total = None
        for start, copy in zip(range(0, points, width), copies):
            copy.wait()
            part = pl.ds(start, width)
            block = kernel_ref.at[:, part]
            piece = column_sums(block, points_of(block, None, mass_ref.at[:, part]))
            total = piece if total is None else total + piece
        sums.append(total)
    send(out_ref, *sums)


def step_kernel(*refs, count, first, fresh, keep):
    refs = list(refs)
    if first:
        cloud_x_ref, cloud_y_ref = refs[:2]
        del refs[:2]
    parts_ref, weight_ref = refs[:2]
    del refs[:2]
    scale_in = None if fresh else refs.pop(0)
    left_ref, right_ref, mass_x_ref, mass_y_ref, out_ref, scale_ref = refs[:6]
    del refs[:6]
    if fresh and not first:
        rows = weight_ref.shape[0]
        totals = tree_sum(parts_ref)
        weights = cube_root(weight_ref[...] * totals[:rows] * totals[rows:])
        scale_left, scale_right, factors = weights / totals[:rows], weights / totals[rows:], None
    else:
        _, scale_left, scale_right, factors = receive(parts_ref, weight_ref, scale_in, count)
    scale_ref[...] = jnp.concatenate([scale_left, scale_right], axis=0)
    if first:
        new_x_ref, new_y_ref = refs[:2]
        del refs[:2]
        new_x_ref[...] = mass_x_ref[...] * factors[0]
        new_y_ref[...] = mass_y_ref[...] * factors[1]
        mass_x_ref, mass_y_ref = new_x_ref, new_y_ref
    point_x_ref, point_y_ref = refs[:2] if keep else (None, None)
    point_x = points_of(left_ref, to_columns(scale_left), mass_x_ref)
    point_y = points_of(right_ref, to_columns(scale_right), mass_y_ref)
    send(out_ref, column_sums(left_ref, point_x), column_sums(right_ref, point_y))
    if keep:
        point_x_ref[...] = point_x
        point_y_ref[...] = point_y
    if first:
        halve_cloud(cloud_x_ref, refs[0], refs[1], 0)
        halve_cloud(cloud_y_ref, refs[2], refs[3], STATS)


def halve_cloud(cloud_ref, tall_ref, flat_ref, place):
    dim, width = cloud_ref.shape[0], 4 * LANES
    lines = lax.broadcasted_iota(jnp.int32, (2 * STATS, width), 0) - place
    ones = jnp.where(lax.broadcasted_iota(jnp.int32, (dim, width), 0) < 3, 1.0, 0.0).astype(HALF)
    for start in range(0, cloud_ref.shape[1], width):
        part = pl.ds(start, width)
        points = cloud_ref[:, part]
        high, low = halves(points)
        square = jnp.sum(points * points, axis=0, keepdims=True)
        square_high = square.astype(HALF).astype(HIGH)
        stats = jnp.where(lines == 1, square - square_high, jnp.where(lines == 2, 1.0, 0.0))
        stats = jnp.where(lines == 0, square_high, stats).astype(HALF)
        tall_ref[:, part] = jnp.concatenate([high, low, stats], axis=0)
        flat_ref[:, part] = jnp.concatenate([high, low, high, ones], axis=0)


def moment_side(kernel_ref, column, mass_ref, tall_ref, plan_ref, width):
    total = None
    for start in range(0, kernel_ref.shape[1], width):
        part = pl.ds(start, width)
        scaled = kernel_ref[:, part] * wide(column, width)
        plan = scaled * (mass_ref[:, part] / jnp.sum(scaled, axis=0, keepdims=True))
        plan_ref[:, part] = plan
        high, low = halves(plan)
        tall = tall_ref[:, part]
        piece = lax.dot_general(tall, high, (((1,), (1,)), ((), ())), preferred_element_type=HIGH)
        piece = piece + lax.dot_general(tall, low, (((1,), (1,)), ((), ())), preferred_element_type=HIGH)
        total = piece if total is None else total + piece
    return total


def moment_kernel(
    parts_ref, weight_ref, scale_ref, left_ref, right_ref, mass_x_ref, mass_y_ref, tall_x_ref, tall_y_ref,
    out_ref, plan_left_ref, plan_right_ref, *, width, count, dim,
):
    _, scale_left, scale_right, _ = receive(parts_ref, weight_ref, scale_ref, count)
    left = moment_side(left_ref, to_columns(scale_left), mass_x_ref, tall_x_ref, plan_left_ref, width)
    right = moment_side(right_ref, to_columns(scale_right), mass_y_ref, tall_y_ref, plan_right_ref, width)
    ranks = left_ref.shape[0]
    products = jnp.concatenate([x[:dim] + x[dim : 2 * dim] for x in (left, right)], axis=0)
    extra = left[2 * dim :] + right[2 * dim :]
    used = ranks
    for j in range(0, ranks, LANES):
        out_ref[j : j + LANES] = jnp.transpose(products[:, j : j + LANES])
        out_ref[used : used + 2 * STATS] = extra[:, j : j + LANES]
        used += 2 * STATS
    if used < out_ref.shape[0]:
        out_ref[used:] = jnp.zeros((out_ref.shape[0] - used, LANES), HIGH)


def mirror_kernel(
    sums_ref, weight_ref, plan_left_ref, plan_right_ref, mass_x_ref, mass_y_ref, flat_x_ref, flat_y_ref,
    out_ref, left_ref, right_ref, weight_out_ref, *, width, dim,
):
    ranks = plan_left_ref.shape[0]
    tiles = ranks // LANES
    lane = lax.broadcasted_iota(jnp.int32, (ranks, LANES), 1)
    lines = [sums_ref[ranks + 2 * STATS * j : ranks + 2 * STATS * (j + 1)] for j in range(tiles)]

    def line(j):
        return jnp.concatenate([x[j : j + 1] for x in lines], axis=0)

    square_left, column_left = line(0) + line(1), line(2)
    square_right, column_right = line(STATS) + line(STATS + 1), line(STATS + 2)
    weights = cube_root(weight_ref[...] * column_left * column_right)
    inverse_left, inverse_right = 1.0 / column_left, 1.0 / column_right
    grad_r, grad_q = square_left * inverse_left, square_right * inverse_right

    def centred(rows):
        return rows - jnp.sum(rows, keepdims=True) * (1.0 / ranks)

    def parts_of(shift):
        shift = shift * (-step_size * LOG2_E)
        high = shift.astype(HALF).astype(HIGH)
        low = (shift - high).astype(HALF).astype(HIGH)
        return high, low, shift - high - low

    def columns(first, second):
        def group(rows, j):
            empty = jnp.zeros((dim - len(rows), LANES), HIGH)
            return [x[j : j + 1] for x in rows] + [empty]

        return jnp.concatenate(
            [jnp.transpose(jnp.concatenate(group(first, j) + group(second, j), axis=0)) for j in range(tiles)],
            axis=0,
        )

    extra = columns(
        (inverse_left, inverse_right, weights * inverse_left, weights * inverse_right), parts_of(centred(grad_q))
    )
    extra_right = columns((), parts_of(centred(grad_r)))
    mean = sums_ref[:ranks] * jnp.where(lane < dim, extra[:, 0:1], extra[:, 1:2])
    swapped = pltpu.roll(mean, dim, 1)
    cross = jnp.broadcast_to(jnp.sum(mean * swapped, axis=1, keepdims=True), (ranks, LANES))
    cross = jnp.concatenate(
        [jnp.transpose(cross[j * LANES : (j + 1) * LANES])[:1] for j in range(tiles)], axis=0
    )
    weight_out_ref[...] = weights * jnp.exp(-step_size * centred(cross - grad_r - grad_q))

    def fields(points, shift, flat_ref, kernel_ref):
        points = points * (2.0 * step_size * LOG2_E)
        high = points.astype(HALF)
        rest = jnp.where(lane < dim, points - high.astype(HIGH), shift).astype(HALF)
        points = jnp.concatenate([high, rest], axis=1)
        for start in range(0, kernel_ref.shape[1], width):
            part = pl.ds(start, width)
            kernel_ref[:, part] = jnp.dot(points, flat_ref[:, part], preferred_element_type=HIGH)

    def advance(factor, plan_ref, mass_ref, kernel_ref):
        factor = jnp.broadcast_to(factor, (ranks, LANES))
        sums = []
        for start in range(0, kernel_ref.shape[1], LANES):
            part = pl.ds(start, LANES)
            kernel = plan_ref[:, part] * factor * jnp.exp2(kernel_ref[:, part])
            kernel_ref[:, part] = kernel
            sums.append(mass_ref[:, part] / jnp.sum(kernel, axis=0, keepdims=True))
        return jnp.concatenate(sums, axis=1)

    fields(jnp.where(lane < dim, swapped, mean), extra, flat_x_ref, left_ref)
    fields(jnp.where(lane < dim, mean, swapped), extra_right, flat_y_ref, right_ref)
    left = advance(extra[:, 2:3], plan_left_ref, mass_x_ref, left_ref)
    right = advance(extra[:, 3:4], plan_right_ref, mass_y_ref, right_ref)
    send(out_ref, column_sums(left_ref, left), column_sums(right_ref, right))


def combine_kernel(parts_ref, out_ref):
    out_ref[...] = jnp.broadcast_to(jnp.sum(parts_ref[...], axis=0, keepdims=True), out_ref.shape)


def last_kernel(
    parts_ref, weight_ref, scale_ref, left_ref, right_ref, point_x_ref, point_y_ref,
    left_hbm, right_hbm, weight_out_ref, left_out, right_out, sems, *, count, height,
):
    ranks = left_ref.shape[0]
    weights, scale_left, scale_right, _ = receive(parts_ref, weight_ref, scale_ref, count)
    copies = []
    for scale, point_ref, kernel_ref, buffer, target in (
        (scale_left, point_x_ref, left_ref, left_out, left_hbm),
        (scale_right, point_y_ref, right_ref, right_out, right_hbm),
    ):
        column = to_columns(scale) * float(RANK)
        for start in range(0, ranks, height):
            part = pl.ds(start, height)
            factor = wide(column[start : start + height], kernel_ref.shape[1])
            buffer[part] = point_ref[...] * kernel_ref[part] * factor
            copies.append(pltpu.make_async_copy(buffer.at[part], target.at[part], sems.at[len(copies)]))
            copies[-1].start()
    weight_out_ref[...] = weights * (RANK / count)
    for copy in copies:
        copy.wait()


def kernel_shards(cloud_x, cloud_y, mass_x, mass_y, left_start, right_start, weight_start):
    ranks, points = left_start.shape
    dim = cloud_x.shape[0]
    devices = lax.axis_size("dp")
    count = float(points * devices)
    tiles = ranks // LANES
    shape = jax.ShapeDtypeStruct
    small = shape((devices, 2 * tiles, LANES), HIGH)
    scale = shape((2 * tiles, LANES), HIGH)
    weight_shape = shape((tiles, LANES), HIGH)
    line = shape((1, points), HIGH)
    matrix = shape((ranks, points), HIGH)
    lines = -(-(ranks + 2 * STATS * tiles) // devices) * devices
    step_width = 512
    width = 256
    height = LANES // 4
    vmem_bytes = 16 * 1024 * 1024

    def call(body, out, *operands, flops, far_in=0, far_out=0, scratch=(), flags=None):
        near, far = pl.BlockSpec(memory_space=pltpu.VMEM), pl.BlockSpec(memory_space=pltpu.HBM)
        spaces = [far] * far_out + [near] * (len(out) - far_out)
        return pl.pallas_call(
            body,
            out_shape=out,
            in_specs=[far] * far_in + [near] * (len(operands) - far_in),
            out_specs=spaces,
            scratch_shapes=scratch,
            compiler_params=pltpu.CompilerParams(vmem_limit_bytes=vmem_bytes, flags=flags),
            cost_estimate=pl.CostEstimate(flops=flops, bytes_accessed=0, transcendentals=0),
        )(*[pltpu.with_memory_space_constraint(x, pltpu.HBM) for x in operands[:far_in]], *operands[far_in:])

    def exchange(sent):
        return lax.all_to_all(sent, "dp", 0, 0)

    step_flops = 8 * ranks * points
    mass_x, mass_y = mass_x.reshape(1, points), mass_y.reshape(1, points)
    weight = weight_start.reshape(tiles, LANES)
    cloud_shapes = (shape((2 * dim + 2 * STATS, points), HALF), shape((4 * dim, points), HALF))
    parts, left, right, mass_x, mass_y = call(
        functools.partial(first_kernel, width=step_width),
        (small, matrix, matrix, line, line),
        left_start, right_start, mass_x, mass_y,
        flops=step_flops,
        far_in=4,
        scratch=[pltpu.SemaphoreType.DMA((2 + 2 * points // step_width,))],
    )
    for outer in range(MIRROR + 1):
        scaling = ()
        for repeat in range(1, INNER):
            parts = exchange(parts)
            if repeat == INNER - 1 and outer < MIRROR:
                break
            first = outer == 0 and repeat == 1
            keep = outer == MIRROR and repeat == INNER - 1
            body = functools.partial(
                step_kernel, count=count, first=first, fresh=repeat == 1, keep=keep
            )
            out = (small, scale) + (line, line) * (first + keep) + cloud_shapes * (2 * first)
            clouds = (cloud_x, cloud_y) * first
            parts, new_scaling, *more = call(
                body, out, *clouds, parts, weight, *scaling, left, right, mass_x, mass_y, flops=step_flops
            )
            scaling = (new_scaling,)
            if first:
                mass_x, mass_y, tall_x, flat_x, tall_y, flat_y = more
        if outer == MIRROR:
            break
        sent, left, right = call(
            functools.partial(moment_kernel, width=width, count=count, dim=dim),
            (shape((lines, LANES), HIGH), matrix, matrix),
            parts, weight, *scaling, left, right, mass_x, mass_y, tall_x, tall_y,
            flops=step_flops + 16 * ranks * points * LANES,
        )
        sent = exchange(sent.reshape(devices, 1, -1))
        (sent,) = call(combine_kernel, (shape(sent.shape, HIGH),), sent, flops=lines * LANES)
        sums = exchange(sent).reshape(lines, LANES)
        parts, left, right, weight = call(
            functools.partial(mirror_kernel, width=width, dim=dim),
            (small, matrix, matrix, weight_shape),
            sums, weight, left, right, mass_x, mass_y, flat_x, flat_y,
            flops=step_flops + 16 * ranks * points * dim,
        )
    parts = exchange(parts)
    left, right, weights = call(
        functools.partial(last_kernel, count=count, height=height),
        (matrix, matrix, weight_shape),
        parts, weight, *scaling, left, right, *more,
        flops=step_flops,
        far_out=2,
        scratch=[
            pltpu.VMEM((ranks, points), HIGH),
            pltpu.VMEM((ranks, points), HIGH),
            pltpu.SemaphoreType.DMA((2 * ranks // height,)),
        ],
    )
    return (left, right, weights.reshape(ranks))


def device_program(cloud_x, cloud_y, mass_x, mass_y, left_start, right_start, weight_start):
    ranks, points = left_start.shape
    whole = lax.axis_size("rank") == 1 and cloud_x.shape[0] == LANES // 2
    body = kernel_shards if whole and ranks % LANES == 0 and points % 512 == 0 else shards
    return body(cloud_x, cloud_y, mass_x, mass_y, left_start, right_start, weight_start)


def solution(mesh):
    in_specs = (
        P(None, "dp"),
        P(None, "dp"),
        P("dp"),
        P("dp"),
        P("rank", "dp"),
        P("rank", "dp"),
        P("rank"),
    )
    out_specs = (P("rank", "dp"), P("rank", "dp"), P("rank"))
    return jax.shard_map(device_program, mesh=mesh, in_specs=in_specs, out_specs=out_specs, check_vma=False)
```

```python
import functools

import jax
import jax.numpy as jnp
from jax import lax
from jax.experimental import pallas as pl
from jax.experimental.pallas import tpu as pltpu
from jax.sharding import PartitionSpec as P

RANK = 256
INNER = 4
MIRROR = 3


exact_mode = lax.Precision.HIGHEST
step_size = 2.0


def total_small(part):
    count = lax.axis_size("dp")
    parts = lax.all_to_all(jnp.broadcast_to(part[None], (count,) + part.shape), "dp", 0, 0)
    return jnp.sum(parts, axis=0)


def total_large(part):
    count = lax.axis_size("dp")
    size = part.shape[0]
    piece = -(-size // (count * 128)) * 128
    padded = jnp.pad(part, (0, piece * count - size)).reshape(count, 1, piece)
    mine = jnp.sum(lax.all_to_all(padded, "dp", 0, 0), axis=0)
    parts = lax.all_to_all(jnp.broadcast_to(mine[None], (count, 1, piece)), "dp", 0, 0)
    return parts.reshape(-1)[:size]


def over_rank(value):
    return lax.psum(value, "rank") if lax.axis_size("rank") > 1 else value


def shards(cloud_x, cloud_y, mass_x, mass_y, left_start, right_start, weight_start):
    ranks_local = left_start.shape[0]
    points_dev = left_start.shape[1]
    dim = cloud_x.shape[0]
    total_count = float(points_dev * lax.axis_size("dp"))
    square_x = jnp.sum(cloud_x * cloud_x, axis=0)
    square_y = jnp.sum(cloud_y * cloud_y, axis=0)

    def rows(scale, kernel):
        return over_rank(jnp.sum(scale[:, None] * kernel, axis=0))

    def columns(kernel, point):
        return jnp.sum(kernel * point[None, :], axis=1)

    left_mass, right_mass = mass_x, mass_y
    kernel_left, kernel_right, kernel_weight = left_start, right_start, weight_start
    for outer in range(MIRROR + 1):
        scale_left = jnp.ones((ranks_local,), jnp.float32)
        scale_right = jnp.ones((ranks_local,), jnp.float32)
        for repeat in range(INNER):
            point_left = left_mass / rows(scale_left, kernel_left)
            point_right = right_mass / rows(scale_right, kernel_right)
            if repeat == INNER - 1 and outer < MIRROR:
                break
            column_left = columns(kernel_left, point_left)
            column_right = columns(kernel_right, point_right)
            if outer == 0 and repeat == 0:
                sums = jnp.stack([jnp.sum(mass_x), jnp.sum(mass_y)])
                packed = total_small(jnp.concatenate([column_left, column_right, sums])[None])[0]
                factor_x = total_count / packed[2 * ranks_local]
                factor_y = total_count / packed[2 * ranks_local + 1]
                left_mass = mass_x * factor_x
                right_mass = mass_y * factor_y
                column_left = packed[:ranks_local] * factor_x
                column_right = packed[ranks_local : 2 * ranks_local] * factor_y
            else:
                packed = total_small(jnp.concatenate([column_left, column_right])[None])[0]
                column_left = packed[:ranks_local]
                column_right = packed[ranks_local:]
            weights = jnp.cbrt(
                kernel_weight * scale_left * column_left * scale_right * column_right
            )
            scale_left = weights / column_left
            scale_right = weights / column_right
        if outer == MIRROR:
            break
        plan_left = kernel_left * point_left[None, :] * scale_left[:, None]
        plan_right = kernel_right * point_right[None, :] * scale_right[:, None]
        packed = total_large(
            jnp.concatenate(
                [
                    jnp.dot(cloud_x, plan_left.T, precision=exact_mode).reshape(-1),
                    jnp.dot(cloud_y, plan_right.T, precision=exact_mode).reshape(-1),
                    jnp.sum(plan_left * square_x[None, :], axis=1),
                    jnp.sum(plan_right * square_y[None, :], axis=1),
                    jnp.sum(plan_left, axis=1),
                    jnp.sum(plan_right, axis=1),
                ]
            )
        )
        packed = packed.reshape(2 * dim + 4, ranks_local)
        column_left, column_right = packed[2 * dim + 2], packed[2 * dim + 3]
        weights = jnp.cbrt(kernel_weight * column_left * column_right)
        mean_x = packed[:dim] / column_left
        mean_y = packed[dim : 2 * dim] / column_right
        grad_q = packed[2 * dim + 1] / column_right
        grad_r = packed[2 * dim] / column_left
        grad_g = -(grad_r + grad_q - 2.0 * jnp.sum(mean_x * mean_y, axis=0))
        centre = over_rank(jnp.stack([jnp.sum(grad_q), jnp.sum(grad_r), jnp.sum(grad_g)])) / RANK
        field_q = (grad_q - centre[0])[:, None] - 2.0 * jnp.dot(mean_y.T, cloud_x, precision=exact_mode)
        field_r = (grad_r - centre[1])[:, None] - 2.0 * jnp.dot(mean_x.T, cloud_y, precision=exact_mode)
        kernel_left = plan_left * (weights / column_left)[:, None] * jnp.exp(-step_size * field_q)
        kernel_right = plan_right * (weights / column_right)[:, None] * jnp.exp(-step_size * field_r)
        kernel_weight = weights * jnp.exp(-step_size * (grad_g - centre[2]))
    left = point_left[None, :] * kernel_left * scale_left[:, None]
    right = point_right[None, :] * kernel_right * scale_right[:, None]
    return (RANK * left, RANK * right, weights * (RANK / total_count))


LANES = 128
HIGH = jnp.float32
HALF = jnp.bfloat16
LOG2_E = 1.4426950408889634
STATS = 8
SMALLEST = 2.0**-126


def halves(value):
    high = value.astype(HALF)
    return high, (value - high.astype(HIGH)).astype(HALF)


def cube_root(value):
    inverse = jnp.exp2(jnp.log2(value) * (-1.0 / 3.0))
    scaled = value * inverse
    inverse = inverse + inverse * (1.0 - scaled * inverse * inverse) * (1.0 / 3.0)
    return jnp.where(value < SMALLEST, 0.0, value * inverse * inverse)


def tree_sum(ref):
    parts = [ref[j] for j in range(ref.shape[0])]
    while len(parts) > 1:
        pairs = [parts[j] + parts[j + 1] for j in range(0, len(parts) - 1, 2)]
        parts = pairs + parts[len(parts) - len(parts) % 2 :]
    return parts[0]


def to_columns(rows):
    return jnp.concatenate(
        [jnp.transpose(jnp.broadcast_to(rows[j : j + 1], (LANES, LANES))) for j in range(rows.shape[0])],
        axis=0,
    )


def to_rows(block):
    return jnp.concatenate(
        [
            jnp.sum(jnp.transpose(block[j : j + LANES]), axis=0, keepdims=True)
            for j in range(0, block.shape[0], LANES)
        ],
        axis=0,
    )


def wide(column, width):
    return jnp.concatenate([column] * (width // LANES), axis=1)


def fold(block):
    total = block[:, :LANES]
    for j in range(LANES, block.shape[1], LANES):
        total = total + block[:, j : j + LANES]
    return total


def points_of(kernel_ref, column, mass_ref):
    points = []
    for start in range(0, kernel_ref.shape[1], LANES):
        part = pl.ds(start, LANES)
        block = kernel_ref[:, part]
        if column is not None:
            block = block * column
        points.append(mass_ref[:, part] / jnp.sum(block, axis=0, keepdims=True))
    return jnp.concatenate(points, axis=1)


def column_sums(kernel_ref, point):
    spread = jnp.broadcast_to(point, (8, point.shape[1]))
    return jnp.concatenate(
        [fold(kernel_ref[pl.ds(row, 8), :] * spread) for row in range(0, kernel_ref.shape[0], 8)], axis=0
    )


def send(out_ref, left, right):
    packed = jnp.concatenate([to_rows(left), to_rows(right)], axis=0)
    out_ref[...] = jnp.broadcast_to(packed[None], out_ref.shape)


def receive(parts_ref, weight_ref, scale_ref, count):
    rows = weight_ref.shape[0]
    totals = tree_sum(parts_ref)
    column_left, column_right = totals[:rows], totals[rows:]
    factors = None
    if scale_ref is None:
        factors = [count / jnp.sum(c, keepdims=True) for c in (column_left, column_right)]
        column_left = column_left * factors[0]
        column_right = column_right * factors[1]
        weights = cube_root(weight_ref[...] * column_left * column_right)
    else:
        weights = cube_root(
            weight_ref[...] * scale_ref[:rows] * column_left * scale_ref[rows:] * column_right
        )
    return weights, weights / column_left, weights / column_right, factors


def first_kernel(
    left_hbm, right_hbm, mass_x_hbm, mass_y_hbm, out_ref, left_ref, right_ref, mass_x_ref, mass_y_ref, sems, *, width
):
    points = left_ref.shape[1]
    small = [
        pltpu.make_async_copy(mass_x_hbm, mass_x_ref, sems.at[0]),
        pltpu.make_async_copy(mass_y_hbm, mass_y_ref, sems.at[1]),
    ]
    large = []
    for source, target in ((left_hbm, left_ref), (right_hbm, right_ref)):
        for start in range(0, points, width):
            part = pl.ds(start, width)
            sem = sems.at[2 + len(large)]
            large.append(pltpu.make_async_copy(source.at[:, part], target.at[:, part], sem))
    for copy in small + large:
        copy.start()
    for copy in small:
        copy.wait()
    half = len(large) // 2
    sums = []
    for kernel_ref, mass_ref, copies in (
        (left_ref, mass_x_ref, large[:half]),
        (right_ref, mass_y_ref, large[half:]),
    ):
        total = None
        for start, copy in zip(range(0, points, width), copies):
            copy.wait()
            part = pl.ds(start, width)
            block = kernel_ref.at[:, part]
            piece = column_sums(block, points_of(block, None, mass_ref.at[:, part]))
            total = piece if total is None else total + piece
        sums.append(total)
    send(out_ref, *sums)


def step_kernel(*refs, count, first, fresh, keep):
    refs = list(refs)
    if first:
        cloud_x_ref, cloud_y_ref = refs[:2]
        del refs[:2]
    parts_ref, weight_ref = refs[:2]
    del refs[:2]
    scale_in = None if fresh else refs.pop(0)
    left_ref, right_ref, mass_x_ref, mass_y_ref, out_ref, scale_ref = refs[:6]
    del refs[:6]
    if fresh and not first:
        rows = weight_ref.shape[0]
        totals = tree_sum(parts_ref)
        weights = cube_root(weight_ref[...] * totals[:rows] * totals[rows:])
        scale_left, scale_right, factors = weights / totals[:rows], weights / totals[rows:], None
    else:
        _, scale_left, scale_right, factors = receive(parts_ref, weight_ref, scale_in, count)
    scale_ref[...] = jnp.concatenate([scale_left, scale_right], axis=0)
    if first:
        new_x_ref, new_y_ref = refs[:2]
        del refs[:2]
        new_x_ref[...] = mass_x_ref[...] * factors[0]
        new_y_ref[...] = mass_y_ref[...] * factors[1]
        mass_x_ref, mass_y_ref = new_x_ref, new_y_ref
    point_x_ref, point_y_ref = refs[:2] if keep else (None, None)
    point_x = points_of(left_ref, to_columns(scale_left), mass_x_ref)
    point_y = points_of(right_ref, to_columns(scale_right), mass_y_ref)
    send(out_ref, column_sums(left_ref, point_x), column_sums(right_ref, point_y))
    if keep:
        point_x_ref[...] = point_x
        point_y_ref[...] = point_y
    if first:
        halve_cloud(cloud_x_ref, refs[0], refs[1], 0)
        halve_cloud(cloud_y_ref, refs[2], refs[3], STATS)


def halve_cloud(cloud_ref, tall_ref, flat_ref, place):
    dim, width = cloud_ref.shape[0], 4 * LANES
    lines = lax.broadcasted_iota(jnp.int32, (2 * STATS, width), 0) - place
    ones = jnp.where(lax.broadcasted_iota(jnp.int32, (dim, width), 0) < 3, 1.0, 0.0).astype(HALF)
    for start in range(0, cloud_ref.shape[1], width):
        part = pl.ds(start, width)
        points = cloud_ref[:, part]
        high, low = halves(points)
        square = jnp.sum(points * points, axis=0, keepdims=True)
        square_high = square.astype(HALF).astype(HIGH)
        stats = jnp.where(lines == 1, square - square_high, jnp.where(lines == 2, 1.0, 0.0))
        stats = jnp.where(lines == 0, square_high, stats).astype(HALF)
        tall_ref[:, part] = jnp.concatenate([high, low, stats], axis=0)
        flat_ref[:, part] = jnp.concatenate([high, low, high, ones], axis=0)


def moment_side(kernel_ref, column, mass_ref, tall_ref, plan_ref, width):
    total = None
    for start in range(0, kernel_ref.shape[1], width):
        part = pl.ds(start, width)
        scaled = kernel_ref[:, part] * wide(column, width)
        plan = scaled * (mass_ref[:, part] / jnp.sum(scaled, axis=0, keepdims=True))
        plan_ref[:, part] = plan
        high, low = halves(plan)
        tall = tall_ref[:, part]
        piece = lax.dot_general(tall, high, (((1,), (1,)), ((), ())), preferred_element_type=HIGH)
        piece = piece + lax.dot_general(tall, low, (((1,), (1,)), ((), ())), preferred_element_type=HIGH)
        total = piece if total is None else total + piece
    return total


def moment_kernel(
    parts_ref, weight_ref, scale_ref, left_ref, right_ref, mass_x_ref, mass_y_ref, tall_x_ref, tall_y_ref,
    out_ref, plan_left_ref, plan_right_ref, *, width, count, dim,
):
    _, scale_left, scale_right, _ = receive(parts_ref, weight_ref, scale_ref, count)
    left = moment_side(left_ref, to_columns(scale_left), mass_x_ref, tall_x_ref, plan_left_ref, width)
    right = moment_side(right_ref, to_columns(scale_right), mass_y_ref, tall_y_ref, plan_right_ref, width)
    ranks = left_ref.shape[0]
    products = jnp.concatenate([x[:dim] + x[dim : 2 * dim] for x in (left, right)], axis=0)
    extra = left[2 * dim :] + right[2 * dim :]
    used = ranks
    for j in range(0, ranks, LANES):
        out_ref[j : j + LANES] = jnp.transpose(products[:, j : j + LANES])
        out_ref[used : used + 2 * STATS] = extra[:, j : j + LANES]
        used += 2 * STATS
    if used < out_ref.shape[0]:
        out_ref[used:] = jnp.zeros((out_ref.shape[0] - used, LANES), HIGH)


def mirror_kernel(
    sums_ref, weight_ref, plan_left_ref, plan_right_ref, mass_x_ref, mass_y_ref, flat_x_ref, flat_y_ref,
    out_ref, left_ref, right_ref, weight_out_ref, *, width, dim,
):
    ranks = plan_left_ref.shape[0]
    tiles = ranks // LANES
    lane = lax.broadcasted_iota(jnp.int32, (ranks, LANES), 1)
    lines = [sums_ref[ranks + 2 * STATS * j : ranks + 2 * STATS * (j + 1)] for j in range(tiles)]

    def line(j):
        return jnp.concatenate([x[j : j + 1] for x in lines], axis=0)

    square_left, column_left = line(0) + line(1), line(2)
    square_right, column_right = line(STATS) + line(STATS + 1), line(STATS + 2)
    weights = cube_root(weight_ref[...] * column_left * column_right)
    inverse_left, inverse_right = 1.0 / column_left, 1.0 / column_right
    grad_r, grad_q = square_left * inverse_left, square_right * inverse_right

    def centred(rows):
        return rows - jnp.sum(rows, keepdims=True) * (1.0 / ranks)

    def parts_of(shift):
        shift = shift * (-step_size * LOG2_E)
        high = shift.astype(HALF).astype(HIGH)
        low = (shift - high).astype(HALF).astype(HIGH)
        return high, low, shift - high - low

    def columns(first, second):
        def group(rows, j):
            empty = jnp.zeros((dim - len(rows), LANES), HIGH)
            return [x[j : j + 1] for x in rows] + [empty]

        return jnp.concatenate(
            [jnp.transpose(jnp.concatenate(group(first, j) + group(second, j), axis=0)) for j in range(tiles)],
            axis=0,
        )

    extra = columns(
        (inverse_left, inverse_right, weights * inverse_left, weights * inverse_right), parts_of(centred(grad_q))
    )
    extra_right = columns((), parts_of(centred(grad_r)))
    mean = sums_ref[:ranks] * jnp.where(lane < dim, extra[:, 0:1], extra[:, 1:2])
    swapped = pltpu.roll(mean, dim, 1)
    cross = jnp.broadcast_to(jnp.sum(mean * swapped, axis=1, keepdims=True), (ranks, LANES))
    cross = jnp.concatenate(
        [jnp.transpose(cross[j * LANES : (j + 1) * LANES])[:1] for j in range(tiles)], axis=0
    )
    weight_out_ref[...] = weights * jnp.exp(-step_size * centred(cross - grad_r - grad_q))

    def fields(points, shift, flat_ref, kernel_ref):
        points = points * (2.0 * step_size * LOG2_E)
        high = points.astype(HALF)
        rest = jnp.where(lane < dim, points - high.astype(HIGH), shift).astype(HALF)
        points = jnp.concatenate([high, rest], axis=1)
        for start in range(0, kernel_ref.shape[1], width):
            part = pl.ds(start, width)
            kernel_ref[:, part] = jnp.dot(points, flat_ref[:, part], preferred_element_type=HIGH)

    def advance(factor, plan_ref, mass_ref, kernel_ref):
        factor = jnp.broadcast_to(factor, (ranks, LANES))
        sums = []
        for start in range(0, kernel_ref.shape[1], LANES):
            part = pl.ds(start, LANES)
            kernel = plan_ref[:, part] * factor * jnp.exp2(kernel_ref[:, part])
            kernel_ref[:, part] = kernel
            sums.append(mass_ref[:, part] / jnp.sum(kernel, axis=0, keepdims=True))
        return jnp.concatenate(sums, axis=1)

    fields(jnp.where(lane < dim, swapped, mean), extra, flat_x_ref, left_ref)
    fields(jnp.where(lane < dim, mean, swapped), extra_right, flat_y_ref, right_ref)
    left = advance(extra[:, 2:3], plan_left_ref, mass_x_ref, left_ref)
    right = advance(extra[:, 3:4], plan_right_ref, mass_y_ref, right_ref)
    send(out_ref, column_sums(left_ref, left), column_sums(right_ref, right))


def combine_kernel(parts_ref, out_ref):
    out_ref[...] = jnp.broadcast_to(jnp.sum(parts_ref[...], axis=0, keepdims=True), out_ref.shape)


def last_kernel(
    parts_ref, weight_ref, scale_ref, left_ref, right_ref, point_x_ref, point_y_ref,
    left_hbm, right_hbm, weight_out_ref, left_out, right_out, sems, *, count, height,
):
    ranks = left_ref.shape[0]
    weights, scale_left, scale_right, _ = receive(parts_ref, weight_ref, scale_ref, count)
    copies = []
    for scale, point_ref, kernel_ref, buffer, target in (
        (scale_left, point_x_ref, left_ref, left_out, left_hbm),
        (scale_right, point_y_ref, right_ref, right_out, right_hbm),
    ):
        column = to_columns(scale) * float(RANK)
        for start in range(0, ranks, height):
            part = pl.ds(start, height)
            factor = wide(column[start : start + height], kernel_ref.shape[1])
            buffer[part] = point_ref[...] * kernel_ref[part] * factor
            copies.append(pltpu.make_async_copy(buffer.at[part], target.at[part], sems.at[len(copies)]))
            copies[-1].start()
    weight_out_ref[...] = weights * (RANK / count)
    for copy in copies:
        copy.wait()


def kernel_shards(cloud_x, cloud_y, mass_x, mass_y, left_start, right_start, weight_start):
    ranks, points = left_start.shape
    dim = cloud_x.shape[0]
    devices = lax.axis_size("dp")
    count = float(points * devices)
    tiles = ranks // LANES
    shape = jax.ShapeDtypeStruct
    small = shape((devices, 2 * tiles, LANES), HIGH)
    scale = shape((2 * tiles, LANES), HIGH)
    weight_shape = shape((tiles, LANES), HIGH)
    line = shape((1, points), HIGH)
    matrix = shape((ranks, points), HIGH)
    lines = -(-(ranks + 2 * STATS * tiles) // devices) * devices
    step_width = 512
    width = 256
    height = LANES // 2
    vmem_bytes = 16 * 1024 * 1024

    def call(body, out, *operands, flops, far_in=0, far_out=0, scratch=(), flags=None):
        near, far = pl.BlockSpec(memory_space=pltpu.VMEM), pl.BlockSpec(memory_space=pltpu.HBM)
        spaces = [far] * far_out + [near] * (len(out) - far_out)
        return pl.pallas_call(
            body,
            out_shape=out,
            in_specs=[far] * far_in + [near] * (len(operands) - far_in),
            out_specs=spaces,
            scratch_shapes=scratch,
            compiler_params=pltpu.CompilerParams(vmem_limit_bytes=vmem_bytes, flags=flags),
            cost_estimate=pl.CostEstimate(flops=flops, bytes_accessed=0, transcendentals=0),
        )(*[pltpu.with_memory_space_constraint(x, pltpu.HBM) for x in operands[:far_in]], *operands[far_in:])

    def exchange(sent):
        return lax.all_to_all(sent, "dp", 0, 0)

    step_flops = 8 * ranks * points
    mass_x, mass_y = mass_x.reshape(1, points), mass_y.reshape(1, points)
    weight = weight_start.reshape(tiles, LANES)
    cloud_shapes = (shape((2 * dim + 2 * STATS, points), HALF), shape((4 * dim, points), HALF))
    parts, left, right, mass_x, mass_y = call(
        functools.partial(first_kernel, width=step_width),
        (small, matrix, matrix, line, line),
        left_start, right_start, mass_x, mass_y,
        flops=step_flops,
        far_in=4,
        scratch=[pltpu.SemaphoreType.DMA((2 + 2 * points // step_width,))],
    )
    for outer in range(MIRROR + 1):
        scaling = ()
        for repeat in range(1, INNER):
            parts = exchange(parts)
            if repeat == INNER - 1 and outer < MIRROR:
                break
            first = outer == 0 and repeat == 1
            keep = outer == MIRROR and repeat == INNER - 1
            body = functools.partial(
                step_kernel, count=count, first=first, fresh=repeat == 1, keep=keep
            )
            out = (small, scale) + (line, line) * (first + keep) + cloud_shapes * (2 * first)
            clouds = (cloud_x, cloud_y) * first
            parts, new_scaling, *more = call(
                body, out, *clouds, parts, weight, *scaling, left, right, mass_x, mass_y, flops=step_flops
            )
            scaling = (new_scaling,)
            if first:
                mass_x, mass_y, tall_x, flat_x, tall_y, flat_y = more
        if outer == MIRROR:
            break
        sent, left, right = call(
            functools.partial(moment_kernel, width=width, count=count, dim=dim),
            (shape((lines, LANES), HIGH), matrix, matrix),
            parts, weight, *scaling, left, right, mass_x, mass_y, tall_x, tall_y,
            flops=step_flops + 16 * ranks * points * LANES,
        )
        sent = exchange(sent.reshape(devices, 1, -1))
        (sent,) = call(combine_kernel, (shape(sent.shape, HIGH),), sent, flops=lines * LANES)
        sums = exchange(sent).reshape(lines, LANES)
        parts, left, right, weight = call(
            functools.partial(mirror_kernel, width=width, dim=dim),
            (small, matrix, matrix, weight_shape),
            sums, weight, left, right, mass_x, mass_y, flat_x, flat_y,
            flops=step_flops + 16 * ranks * points * dim,
        )
    parts = exchange(parts)
    left, right, weights = call(
        functools.partial(last_kernel, count=count, height=height),
        (matrix, matrix, weight_shape),
        parts, weight, *scaling, left, right, *more,
        flops=step_flops,
        far_out=2,
        scratch=[
            pltpu.VMEM((ranks, points), HIGH),
            pltpu.VMEM((ranks, points), HIGH),
            pltpu.SemaphoreType.DMA((2 * ranks // height,)),
        ],
    )
    return (left, right, weights.reshape(ranks))


def device_program(cloud_x, cloud_y, mass_x, mass_y, left_start, right_start, weight_start):
    ranks, points = left_start.shape
    whole = lax.axis_size("rank") == 1 and cloud_x.shape[0] == LANES // 2
    body = kernel_shards if whole and ranks % LANES == 0 and points % 512 == 0 else shards
    return body(cloud_x, cloud_y, mass_x, mass_y, left_start, right_start, weight_start)


def solution(mesh):
    in_specs = (
        P(None, "dp"),
        P(None, "dp"),
        P("dp"),
        P("dp"),
        P("rank", "dp"),
        P("rank", "dp"),
        P("rank"),
    )
    out_specs = (P("rank", "dp"), P("rank", "dp"), P("rank"))
    return jax.shard_map(device_program, mesh=mesh, in_specs=in_specs, out_specs=out_specs, check_vma=False)
```
